16 devices in a mesh: tp: 2 (over z), dp: 8 (over y, x, core).
Axes of the slice: x: 2, y: 2, z: 2, core: 2. Of those that a mesh axis runs over, the one named last changes fastest.
Arguments:
- feats: bfloat16 [1024, 144, 1536], P('dp')
- ln_gamma: float32 [1536], replicated
- ln_beta: float32 [1536], replicated
- w_head: bfloat16 [1536, 22528], P(None, 'tp')
- b_head: float32 [22528], P('tp')
- labels: int32 [1024], P('dp')
Outputs:
- output 1: float32 [], replicated
- output 2: bfloat16 [1024, 144, 1536], P('dp')
- output 3: float32 [1536, 22528], P(None, 'tp')
- output 4: float32 [22528], P('tp')
- output 5: float32 [1536], replicated
- output 6: float32 [1536], replicated
All inputs are finite; a program needn't handle non-finite values.
Results may differ from the reference program's by a relative error of at most 0.001.
Values sent between devices are 32-bit elements.
A program may use at most 1 GiB of HBM per device.

```python
import jax
import jax.numpy as jnp
from jax import lax

GLOBAL_BATCH = 1024
TOKENS = 144
WIDTH = 1536
CLASSES = 21841
PADDED_CLASSES = 22528
ROW_BLOCK = min(GLOBAL_BATCH, 64)
LN_EPS = 1e-5
SMOOTH = 0.1


def setup_inputs(seed: int = 0) -> dict:
    sub_keys = jax.random.split(jax.random.key(seed), 7)
    image_shared = jax.random.normal(sub_keys[0], (GLOBAL_BATCH, 1, WIDTH), jnp.float32)
    token_noise = jax.random.normal(sub_keys[1], (GLOBAL_BATCH, TOKENS, WIDTH), jnp.float32)
    feats = (image_shared + 0.5 * token_noise).astype(jnp.bfloat16)
    ln_gamma = 1.0 + 0.3 * jax.random.normal(sub_keys[2], (WIDTH,), jnp.float32)
    ln_beta = 0.3 * jax.random.normal(sub_keys[3], (WIDTH,), jnp.float32)
    w_scale = 3.0 * WIDTH ** -0.5
    w_head = (w_scale * jax.random.normal(sub_keys[4], (WIDTH, PADDED_CLASSES), jnp.float32)).astype(jnp.bfloat16)
    b_head = 0.5 * jax.random.normal(sub_keys[5], (PADDED_CLASSES,), jnp.float32)
    labels = jax.random.randint(sub_keys[6], (GLOBAL_BATCH,), 0, CLASSES, dtype=jnp.int32)
    labels = labels.at[0].set(0).at[GLOBAL_BATCH - 1].set(CLASSES - 1)
    return {"feats": feats, "ln_gamma": ln_gamma, "ln_beta": ln_beta, "w_head": w_head, "b_head": b_head, "labels": labels}


def norm_pool(feats, ln_gamma, ln_beta):
    x_val = feats.astype(jnp.float32)
    mean_x = jnp.mean(x_val, axis=-1, keepdims=True)
    centered = x_val - mean_x
    var_x = jnp.mean(centered * centered, axis=-1, keepdims=True)
    inv_std = lax.rsqrt(var_x + LN_EPS)
    x_hat = centered * inv_std
    x_hat_mean = jnp.mean(x_hat, axis=1)
    pooled16 = (x_hat_mean * ln_gamma + ln_beta).astype(jnp.bfloat16)
    return x_hat, inv_std, x_hat_mean, pooled16


def norm_backward(grad_pool, x_hat, inv_std, x_hat_mean, ln_gamma):
    grad_gamma = jnp.sum(grad_pool * x_hat_mean, axis=0)
    grad_beta = jnp.sum(grad_pool, axis=0)
    upstream = grad_pool * ln_gamma / TOKENS
    up_mean = jnp.mean(upstream, axis=-1)
    proj_term = jnp.mean(x_hat * upstream[:, None, :], axis=-1, keepdims=True)
    grad_x = inv_std * (upstream[:, None, :] - up_mean[:, None, None] - x_hat * proj_term)
    return grad_x.astype(jnp.bfloat16), grad_gamma, grad_beta


def head_rows(feat_rows, label_rows, ln_gamma, ln_beta, w_head, b_head):
    x_hat, inv_std, x_hat_mean, pooled16 = norm_pool(feat_rows, ln_gamma, ln_beta)
    col_ids = jnp.arange(PADDED_CLASSES)
    valid_mask = col_ids < CLASSES
    logits = jnp.dot(pooled16, w_head, preferred_element_type=jnp.float32) + b_head
    logits = jnp.where(valid_mask, logits, -1e30)
    row_max = jnp.max(logits, axis=-1, keepdims=True)
    log_norm = row_max + jnp.log(jnp.sum(jnp.exp(logits - row_max), axis=-1, keepdims=True))
    onehot = col_ids == label_rows[:, None]
    target = jnp.sum(jnp.where(onehot, logits, 0.0), axis=-1)
    valid_sum = jnp.sum(jnp.where(valid_mask, logits, 0.0), axis=-1)
    loss_rows = log_norm[:, 0] - (1.0 - SMOOTH) * target - (SMOOTH / CLASSES) * valid_sum
    soft_probs = jnp.exp(logits - log_norm)
    dlogit = (soft_probs - (1.0 - SMOOTH) * onehot - (SMOOTH / CLASSES) * valid_mask) / GLOBAL_BATCH
    dlogit16 = dlogit.astype(jnp.bfloat16)
    grad_w = jnp.dot(pooled16.T, dlogit16, preferred_element_type=jnp.float32)
    grad_b = jnp.sum(dlogit, axis=0)
    grad_pool = jnp.dot(dlogit16, w_head.T, preferred_element_type=jnp.float32)
    grad_x, grad_gamma, grad_beta = norm_backward(grad_pool, x_hat, inv_std, x_hat_mean, ln_gamma)
    return jnp.sum(loss_rows), grad_x, grad_w, grad_b, grad_gamma, grad_beta


def reference(feats, ln_gamma, ln_beta, w_head, b_head, labels):
    block_count = GLOBAL_BATCH // ROW_BLOCK
    feat_blocks = feats.reshape(block_count, ROW_BLOCK, TOKENS, WIDTH)
    label_blocks = labels.reshape(block_count, ROW_BLOCK)
    init_carry = (jnp.zeros((), jnp.float32), jnp.zeros((WIDTH, PADDED_CLASSES), jnp.float32), jnp.zeros((PADDED_CLASSES,), jnp.float32), jnp.zeros((WIDTH,), jnp.float32), jnp.zeros((WIDTH,), jnp.float32))

    def scan_step(acc_carry, block_in):
        loss_sum, grad_x, grad_w, grad_b, grad_gamma, grad_beta = head_rows(block_in[0], block_in[1], ln_gamma, ln_beta, w_head, b_head)
        new_carry = (acc_carry[0] + loss_sum, acc_carry[1] + grad_w, acc_carry[2] + grad_b, acc_carry[3] + grad_gamma, acc_carry[4] + grad_beta)
        return new_carry, grad_x

    final_carry, grad_blocks = lax.scan(scan_step, init_carry, (feat_blocks, label_blocks))
    grad_feats = grad_blocks.reshape(GLOBAL_BATCH, TOKENS, WIDTH)
    return (final_carry[0] / GLOBAL_BATCH, grad_feats, final_carry[1], final_carry[2], final_carry[3], final_carry[4])
```

```python
import functools
import math

import jax
import jax.numpy as jnp
from jax import lax
from jax.experimental import pallas as pl
from jax.experimental.pallas import tpu as pltpu
from jax.sharding import PartitionSpec as P

VALID_CLASSES = 21841
LN_EPS = 1e-5
SMOOTH = 0.1
LANES = 128
COLS = 512
SUB = 256
IMGS = 8
ROW_TILE = 16


def norm_kernel(x_ref, pool_ref, mean_ref, inv_ref):
    imgs, tokens, width = x_ref.shape
    chunks = tokens // ROW_TILE
    lane = lax.broadcasted_iota(jnp.int32, (ROW_TILE, LANES), 1)

    def one_image(i, carry):
        means, invs = [], []
        for c in range(chunks):
            x = x_ref[i, pl.ds(c * ROW_TILE, ROW_TILE), :].astype(jnp.float32)
            means.append(jnp.sum(x, axis=1, keepdims=True) * (1.0 / width))
        for c in range(chunks):
            x = x_ref[i, pl.ds(c * ROW_TILE, ROW_TILE), :].astype(jnp.float32) - means[c]
            var = jnp.sum(x * x, axis=1, keepdims=True) * (1.0 / width)
            invs.append(lax.rsqrt(var + LN_EPS))
        total = jnp.zeros((ROW_TILE, width), jnp.float32)
        for c in range(chunks):
            x = x_ref[i, pl.ds(c * ROW_TILE, ROW_TILE), :].astype(jnp.float32) - means[c]
            total = total + x * invs[c]
            rows = pl.ds(c * ROW_TILE, ROW_TILE)
            mean_ref[0, rows, :] = jnp.where(lane == i, means[c], mean_ref[0, rows, :])
            inv_ref[0, rows, :] = jnp.where(lane == i, invs[c], inv_ref[0, rows, :])
        pool_ref[pl.ds(i, 1), :] = jnp.sum(total, axis=0, keepdims=True) * (1.0 / tokens)
        return carry

    lax.fori_loop(0, imgs, one_image, 0)


def norm_call(feats):
    rows, tokens, width = feats.shape
    stat = jax.ShapeDtypeStruct((rows // IMGS, tokens, LANES), jnp.float32)
    return pl.pallas_call(
        norm_kernel,
        name="norm_pool",
        grid=(rows // IMGS,),
        in_specs=[pl.BlockSpec((IMGS, tokens, width), lambda g: (g, 0, 0))],
        out_specs=[
            pl.BlockSpec((IMGS, width), lambda g: (g, 0)),
            pl.BlockSpec((1, tokens, LANES), lambda g: (g, 0, 0)),
            pl.BlockSpec((1, tokens, LANES), lambda g: (g, 0, 0)),
        ],
        out_shape=[jax.ShapeDtypeStruct((rows, width), jnp.float32), stat, stat],
        compiler_params=pltpu.CompilerParams(vmem_limit_bytes=48 * 2**20),
        cost_estimate=pl.CostEstimate(flops=10 * rows * tokens * width, bytes_accessed=2 * rows * tokens * width, transcendentals=0),
    )(feats)


def wide(column_tile):
    return jnp.concatenate([column_tile] * (SUB // LANES), axis=1)


def head_block(shard_cols, block, rows_total, p_ref, pt_ref, lse_ref, y_ref, w_ref, b_ref, dw_ref, db_ref, dl_ref):
    rows = p_ref.shape[0]
    base = lax.axis_index("tp") * shard_cols + block * COLS
    for s in range(COLS // SUB):
        sub = pl.ds(s * SUB, SUB)
        logits = jnp.dot(p_ref[...], w_ref[:, sub], preferred_element_type=jnp.float32)
        col = base + s * SUB + lax.broadcasted_iota(jnp.int32, (1, SUB), 1)
        valid = col < VALID_CLASSES
        smooth = jnp.where(valid, SMOOTH / VALID_CLASSES, 0.0)
        target = smooth + (1.0 - SMOOTH)
        bias = jnp.where(valid, b_ref[:, sub], -jnp.inf)
        soft = jnp.exp((logits + bias) - wide(lse_ref[...]))
        dlogit = (soft - jnp.where(wide(y_ref[...]) == col, target, smooth)) * (1.0 / rows_total)
        db_ref[:, sub] = jnp.sum(dlogit, axis=0, keepdims=True)
        dl_ref[s] = dlogit.astype(jnp.bfloat16)
    for s in range(COLS // SUB):
        dw_ref[:, pl.ds(s * SUB, SUB)] = jnp.dot(pt_ref[...], dl_ref[s], preferred_element_type=jnp.float32)


def head_kernel(shard_cols, rows_total, p_ref, pt_ref, lse_ref, y_ref, w_ref, b_ref, dw_ref, db_ref, dl_ref):
    head_block(shard_cols, pl.program_id(0), rows_total, p_ref, pt_ref, lse_ref, y_ref, w_ref, b_ref, dw_ref, db_ref, dl_ref)


def head_feat_kernel(shard_cols, rows_total, first, p_ref, pt_ref, lse_ref, y_ref, w_ref, b_ref, x_ref, mean_ref, inv_ref, u_ref, um_ref, dw_in, db_in, dw_ref, db_ref, df_ref, dl_ref):
    imgs, tokens, width = x_ref.shape
    chunks = tokens // ROW_TILE
    for i in range(imgs):
        u = u_ref[pl.ds(i, 1), :]
        um = um_ref[pl.ds(i, 1), :][:, :1]
        for c in range(chunks):
            rows = pl.ds(c * ROW_TILE, ROW_TILE)
            mean = mean_ref[0, rows, pl.ds(i, 1)]
            inv = inv_ref[0, rows, pl.ds(i, 1)]
            x = x_ref[i, rows, :].astype(jnp.float32)
            proj = jnp.sum((x - mean) * u, axis=1, keepdims=True) * (inv * (1.0 / width))
            slope = -(inv * inv * proj)
            offset = -(inv * um) - slope * mean
            x = x_ref[i, rows, :].astype(jnp.float32)
            df_ref[i, rows, :] = (x * slope + (u * inv + offset)).astype(jnp.bfloat16)
    head_block(shard_cols, pl.program_id(0) + first, rows_total, p_ref, pt_ref, lse_ref, y_ref, w_ref, b_ref, dw_ref, db_ref, dl_ref)


def resident(shape):
    return pl.BlockSpec(shape, lambda g: (0,) * len(shape), pipeline_mode=pl.Buffered(1))


def head_specs(rows, width, first):
    return [
        resident((rows, width)),
        resident((width, rows)),
        resident((rows, LANES)),
        resident((rows, LANES)),
        pl.BlockSpec((width, COLS), lambda g: (0, g + first)),
        pl.BlockSpec((1, COLS), lambda g: (0, g + first)),
    ]


def head_calls(p_all, lse_all, y_all, w_head, b_head, feats, mean, inv, make_u):
    rows, width = p_all.shape
    shard_cols = w_head.shape[1]
    imgs_all, tokens, _ = feats.shape
    steps = shard_cols // COLS
    feat_steps = imgs_all // IMGS
    first = steps - feat_steps
    pt_all = p_all.T
    lse_b = jnp.broadcast_to(lse_all[:, None], (rows, LANES))
    y_b = jnp.broadcast_to(y_all[:, None], (rows, LANES))
    b_row = b_head[None, :]
    head_args = (p_all, pt_all, lse_b, y_b, w_head, b_row)
    dw_shape = jax.ShapeDtypeStruct((width, shard_cols), jnp.float32)
    db_shape = jax.ShapeDtypeStruct((1, shard_cols), jnp.float32)
    params = pltpu.CompilerParams(vmem_limit_bytes=60 * 2**20)
    scratch = [pltpu.VMEM((COLS // SUB, rows, SUB), jnp.bfloat16)]

    def cost(n):
        return pl.CostEstimate(flops=4 * rows * width * COLS * n, bytes_accessed=6 * width * COLS * n, transcendentals=rows * COLS * n)

    dw, db = pl.pallas_call(
        functools.partial(head_kernel, shard_cols, rows),
        name="head_first",
        grid=(first,),
        in_specs=head_specs(rows, width, 0),
        out_specs=[pl.BlockSpec((width, COLS), lambda g: (0, g)), pl.BlockSpec((1, COLS), lambda g: (0, g))],
        out_shape=[dw_shape, db_shape],
        scratch_shapes=scratch,
        compiler_params=params,
        cost_estimate=cost(first),
    )(*head_args)
    u, um = make_u()
    um_b = jnp.broadcast_to(um[:, None], (imgs_all, LANES))
    img = lambda shape: pl.BlockSpec(shape, lambda g: (g,) + (0,) * (len(shape) - 1))
    n_in = 11
    dw, db, df = pl.pallas_call(
        functools.partial(head_feat_kernel, shard_cols, rows, first),
        name="head_rest",
        grid=(feat_steps,),
        in_specs=head_specs(rows, width, first)
        + [img((IMGS, tokens, width)), img((1, tokens, LANES)), img((1, tokens, LANES)), img((IMGS, width)), img((IMGS, LANES))]
        + [pl.BlockSpec(memory_space=pl.ANY)] * 2,
        out_specs=[
            pl.BlockSpec((width, COLS), lambda g: (0, g + first)),
            pl.BlockSpec((1, COLS), lambda g: (0, g + first)),
            img((IMGS, tokens, width)),
        ],
        out_shape=[dw_shape, db_shape, jax.ShapeDtypeStruct(feats.shape, jnp.bfloat16)],
        scratch_shapes=scratch,
        input_output_aliases={n_in: 0, n_in + 1: 1},
        compiler_params=params,
        cost_estimate=cost(feat_steps),
    )(*head_args, feats, mean, inv, u, um_b, dw, db)
    return dw, db[0], df


def solution(mesh):
    def local_head(feats, ln_gamma, ln_beta, w_head, b_head, labels):
        shard_cols = w_head.shape[1]
        tokens = feats.shape[1]
        xhat_mean, mean, inv = norm_call(feats)
        pool_all = lax.all_gather(xhat_mean, "dp", axis=0, tiled=True)
        p_all = (pool_all * ln_gamma + ln_beta).astype(jnp.bfloat16)
        y_all = lax.all_gather(labels, "dp", axis=0, tiled=True)
        rows = p_all.shape[0]

        pooled16 = (xhat_mean * ln_gamma + ln_beta).astype(jnp.bfloat16)
        col_ids = lax.axis_index("tp") * shard_cols + jnp.arange(shard_cols)
        valid = col_ids < VALID_CLASSES
        logits = jnp.dot(pooled16, w_head, preferred_element_type=jnp.float32) + b_head
        logits = jnp.where(valid, logits, -1e30)
        row_max = lax.pmax(jnp.max(logits, axis=-1), "tp")
        shifted = jnp.exp(logits - row_max[:, None])
        onehot = col_ids == labels[:, None]
        stats = jnp.stack([jnp.sum(shifted, axis=-1), jnp.sum(jnp.where(onehot, logits, 0.0), axis=-1), jnp.sum(jnp.where(valid, logits, 0.0), axis=-1)])
        stats = lax.psum(stats, "tp")
        lse = row_max + jnp.log(stats[0])
        loss_rows = lse - (1.0 - SMOOTH) * stats[1] - (SMOOTH / VALID_CLASSES) * stats[2]
        lse_all = lax.all_gather(lse, "dp", axis=0, tiled=True)
        soft = shifted / stats[0][:, None]
        dlogit16 = ((soft - (1.0 - SMOOTH) * onehot - (SMOOTH / VALID_CLASSES) * valid) / rows).astype(jnp.bfloat16)
        dpool_part = lax.dot_general(dlogit16, w_head, (((1,), (1,)), ((), ())), preferred_element_type=jnp.float32)
        dpool_other = lax.ppermute(dpool_part, "tp", [(0, 1), (1, 0)])
        small = (jnp.sum(loss_rows), jnp.sum(dpool_part * xhat_mean, axis=0), jnp.sum(dpool_part, axis=0))

        def make_u():
            u = (dpool_part + dpool_other) * ln_gamma / tokens
            return u, jnp.mean(u, axis=-1)

        dw, db, df = head_calls(p_all, lse_all, y_all, w_head, b_head, feats, mean, inv, make_u)
        loss_sum = lax.psum(small[0], "dp")
        dgamma, dbeta = lax.psum((small[1], small[2]), ("dp", "tp"))
        return loss_sum / rows, df, dw, db, dgamma, dbeta

    return jax.shard_map(local_head, mesh=mesh, in_specs=(P("dp", None, None), P(), P(), P(None, "tp"), P("tp"), P("dp")), out_specs=(P(), P("dp", None, None), P(None, "tp"), P("tp"), P(), P()), check_vma=False)
```

```python
import functools
import math

import jax
import jax.numpy as jnp
from jax import lax
from jax.experimental import pallas as pl
from jax.experimental.pallas import tpu as pltpu
from jax.sharding import PartitionSpec as P

VALID_CLASSES = 21841
LN_EPS = 1e-5
SMOOTH = 0.1
LANES = 128
COLS = 512
SUB = 256
IMGS = 8
ROW_TILE = 16
GROUP = 4
WCOLS = 1024
SLOTS = 3


def repeat_lanes(tile, width):
    return jnp.concatenate([tile] * (width // LANES), axis=1)


def fold_lanes(x, op):
    tiles = [x[:, j * LANES:(j + 1) * LANES] for j in range(x.shape[1] // LANES)]
    return functools.reduce(op, tiles)


def spread_row(row):
    return jnp.broadcast_to(row, (LANES, LANES)).T


def norm_image(x_ref, slot, i, lane_id, pool_row, pool_ref, mean_ref, inv_ref):
    _, _, tokens, width = x_ref.shape
    chunks = tokens // ROW_TILE
    lane = lax.broadcasted_iota(jnp.int32, (ROW_TILE, LANES), 1)
    means, invs = [], []
    for c in range(chunks):
        x = x_ref[slot, i, pl.ds(c * ROW_TILE, ROW_TILE), :].astype(jnp.float32)
        means.append(jnp.sum(x, axis=1, keepdims=True) * (1.0 / width))
    for c in range(chunks):
        x = x_ref[slot, i, pl.ds(c * ROW_TILE, ROW_TILE), :].astype(jnp.float32) - means[c]
        var = jnp.sum(x * x, axis=1, keepdims=True) * (1.0 / width)
        invs.append(lax.rsqrt(var + LN_EPS))
    total = jnp.zeros((ROW_TILE, width), jnp.float32)
    shift = jnp.zeros((ROW_TILE, 1), jnp.float32)
    for c in range(chunks):
        x = x_ref[slot, i, pl.ds(c * ROW_TILE, ROW_TILE), :].astype(jnp.float32)
        total = total + x * invs[c]
        shift = shift + means[c] * invs[c]
        rows = pl.ds(c * ROW_TILE, ROW_TILE)
        mean_ref[rows, :] = jnp.where(lane == lane_id, means[c], mean_ref[rows, :])
        inv_ref[rows, :] = jnp.where(lane == lane_id, invs[c], inv_ref[rows, :])
    pool_ref[pl.ds(pool_row, 1), :] = jnp.sum(total - shift, axis=0, keepdims=True) * (1.0 / tokens)


def front_kernel(x_hbm, w_hbm, b_ref, gamma_ref, beta_ref, y_ref,
                 pool_out, mean_ref, inv_ref, dpool_ref, lse_ref, loss_ref, dgb_ref,
                 x_buf, w_buf, pool, logits, p16, stat_send, stat_recv, part, part_all, mi_send, mi_recv,
                 x_sem, w_sem, send_sem, recv_sem, st_send_sem, st_recv_sem, dg_send_sem, dg_recv_sem, out_sem):
    rows, tokens, width = x_hbm.shape
    half = rows // 2
    quarter = half // 2
    shard_cols = w_hbm.shape[1]
    n_w = shard_cols // WCOLS
    groups = half // GROUP
    rows_total = pool.shape[0]
    t = lax.axis_index("tp")
    d = lax.axis_index("dp")
    me = t * 8 + d
    dx = d + 2 - 4 * ((d // 2) % 2)
    dy = d + 4 - 8 * (d // 4)
    dxy = dx + 4 - 8 * (d // 4)

    def sibling(q):
        return q + 1 - 2 * (q % 2)

    def peer(k):
        q = (me + k) % 16
        return {"tp": q // 8, "dp": q % 8}

    barrier = pltpu.get_barrier_semaphore()
    for k in range(1, 16):
        pl.semaphore_signal(barrier, inc=1, device_id=peer(k), device_id_type=pl.DeviceIdType.MESH)

    def x_copy(g, slot):
        return pltpu.make_async_copy(x_hbm.at[pl.ds(t * half + g * GROUP, GROUP)], x_buf.at[slot], x_sem.at[slot])

    def w_copy(k):
        return pltpu.make_async_copy(w_hbm.at[:, pl.ds(k * WCOLS, WCOLS)], w_buf.at[k], w_sem.at[k])

    def chunk(q, tt, h):
        return pool.at[pl.ds(q * rows + tt * half + h * quarter, quarter)]

    def remote(ref, sem, target):
        return pltpu.make_async_remote_copy(src_ref=ref, dst_ref=ref, send_sem=send_sem.at[sem], recv_sem=recv_sem.at[sem], device_id=target, device_id_type=pl.DeviceIdType.MESH)

    to_z = {"tp": 1 - t, "dp": d}
    to_x = {"tp": t, "dp": dx}
    to_y = {"tp": t, "dp": dy}
    to_c = {"tp": t, "dp": sibling(d)}

    x_copy(0, 0).start()
    x_copy(1, 1).start()
    mean_ref[...] = jnp.zeros_like(mean_ref)
    inv_ref[...] = jnp.zeros_like(inv_ref)

    def do_group(g, carry):
        slot = g % SLOTS
        x_copy(g, slot).wait()

        @pl.when(g + 2 < groups)
        def _():
            x_copy(g + 2, (g + 2) % SLOTS).start()

        @pl.when(g < n_w)
        def _():
            w_copy(g).start()

        def image(i, c):
            local = t * half + g * GROUP + i
            norm_image(x_buf, slot, i, local, d * rows + local, pool, mean_ref, inv_ref)
            return c

        lax.fori_loop(0, GROUP, image, 0)
        return carry

    lax.fori_loop(0, groups // 2, do_group, 0)
    pl.semaphore_wait(barrier, 15)
    first = [[remote(chunk(d, t, h), 3 * h + j, to) for j, to in enumerate((to_z, to_x, to_y))] for h in range(2)]
    for c in first[0]:
        c.start()
    lax.fori_loop(groups // 2, groups, do_group, 0)
    mi_send[0] = mean_ref[...]
    mi_send[1] = inv_ref[...]
    for c in first[1]:
        c.start()
    mi_copy = pltpu.make_async_remote_copy(src_ref=mi_send, dst_ref=mi_recv, send_sem=send_sem.at[18], recv_sem=recv_sem.at[18], device_id=to_z, device_id_type=pl.DeviceIdType.MESH)
    second = [[remote(chunk(d, 1 - t, h), 6 + 2 * h + j, to) for j, to in enumerate((to_x, to_y))] for h in range(2)]
    third = [[remote(chunk(dx, t, h), 10 + 2 * h, to_y), remote(chunk(dy, 1 - t, h), 11 + 2 * h, to_x)] for h in range(2)]

    def block(q):
        return pool.at[pl.ds(q * rows, rows)]

    fourth = [remote(block(q), 14 + j, to_c) for j, q in enumerate((d, dx, dy, dxy))]
    for h in range(2):
        first[h][0].wait_recv()
        for c in second[h]:
            c.start()
    fourth[0].start()
    mi_copy.start()

    p16[...] = (pool[pl.ds(d * rows, rows), :] * gamma_ref[...] + beta_ref[...]).astype(jnp.bfloat16)

    def col_ids(k):
        return t * shard_cols + k * WCOLS + lax.broadcasted_iota(jnp.int32, (1, WCOLS), 1)

    def logits_step(k, top):
        w_copy(k).wait()
        cols = col_ids(k)
        bias = jnp.where(cols < VALID_CLASSES, b_ref[k], -jnp.inf)
        out = jnp.dot(p16[...], w_buf[k], preferred_element_type=jnp.float32) + bias
        logits[k] = out
        return jnp.maximum(top, fold_lanes(out, jnp.maximum))

    top = lax.fori_loop(0, n_w, logits_step, jnp.full((rows, LANES), -jnp.inf, jnp.float32))
    for h in range(2):
        first[h][1].wait_recv()
        third[h][0].start()
    for h in range(2):
        second[h][1].wait_recv()
        third[h][1].start()
    for h in range(2):
        second[h][0].wait_recv()
        first[h][2].wait_recv()
    fourth[1].start()
    fourth[2].start()
    row_top = jnp.broadcast_to(jnp.max(top, axis=1, keepdims=True), (rows, LANES))
    labels = y_ref[...]
    zero = jnp.zeros((rows, LANES), jnp.float32)

    def stat_step(k, carry):
        total, target, valid_sum = carry
        cols = col_ids(k)
        out = logits[k]
        e = jnp.exp(out - repeat_lanes(row_top, WCOLS))
        hit = jnp.where(repeat_lanes(labels, WCOLS) == cols, out, 0.0)
        ok = jnp.where(cols < VALID_CLASSES, out, 0.0)
        return total + fold_lanes(e, jnp.add), target + fold_lanes(hit, jnp.add), valid_sum + fold_lanes(ok, jnp.add)

    total, target, valid_sum = lax.fori_loop(0, n_w, stat_step, (zero, zero, zero))
    lane = lax.broadcasted_iota(jnp.int32, (rows, LANES), 1)
    packed = jnp.where(lane == 0, row_top, jnp.where(lane == 1, jnp.sum(total, axis=1, keepdims=True), jnp.where(lane == 2, jnp.sum(target, axis=1, keepdims=True), jnp.sum(valid_sum, axis=1, keepdims=True))))
    stat_send[...] = packed.T[:8]
    stat_recv[me] = stat_send[...]

    def stat_copy(k):
        return pltpu.make_async_remote_copy(src_ref=stat_send, dst_ref=stat_recv.at[me], send_sem=st_send_sem.at[k - 1], recv_sem=st_recv_sem.at[k - 1], device_id=peer(k), device_id_type=pl.DeviceIdType.MESH)

    stat_copies = [stat_copy(k) for k in range(1, 16)]
    for c in stat_copies:
        c.start()
    for c in stat_copies:
        c.wait()

    def lse_of(q):
        a, b = stat_recv[q], stat_recv[8 + q]
        hi = jnp.maximum(a[0:1], b[0:1])
        return hi + jnp.log(a[1:2] * jnp.exp(a[0:1] - hi) + b[1:2] * jnp.exp(b[0:1] - hi))

    loss = jnp.zeros((1, LANES), jnp.float32)
    for q in range(8):
        lse_q = lse_of(q)
        lse_ref[q:q + 1, :] = lse_q
        a, b = stat_recv[q], stat_recv[8 + q]
        loss = loss + lse_q - (1.0 - SMOOTH) * (a[2:3] + b[2:3]) - (SMOOTH / VALID_CLASSES) * (a[3:4] + b[3:4])
    loss_ref[...] = jnp.broadcast_to(loss, loss_ref.shape)
    lse_own = spread_row(lse_of(d))
    dpool_ref[...] = jnp.zeros_like(dpool_ref)

    def dpool_step(k, carry):
        cols = col_ids(k)
        smooth = jnp.where(cols < VALID_CLASSES, SMOOTH / VALID_CLASSES, 0.0)
        soft = jnp.exp(logits[k] - repeat_lanes(lse_own, WCOLS))
        dl = (soft - jnp.where(repeat_lanes(labels, WCOLS) == cols, smooth + (1.0 - SMOOTH), smooth)) * (1.0 / rows_total)
        dpool_ref[...] += lax.dot_general(dl.astype(jnp.bfloat16), w_buf[k], (((1,), (1,)), ((), ())), preferred_element_type=jnp.float32)
        return carry

    lax.fori_loop(0, n_w, dpool_step, 0)
    for h in range(2):
        third[h][0].wait_recv()
        third[h][1].wait_recv()
    fourth[3].start()
    dpool = dpool_ref[...]
    part[0:1, :] = jnp.sum(dpool * pool[pl.ds(d * rows, rows), :], axis=0, keepdims=True)
    part[1:2, :] = jnp.sum(dpool, axis=0, keepdims=True)
    part_all[me] = part[...]

    def part_copy(k):
        return pltpu.make_async_remote_copy(src_ref=part, dst_ref=part_all.at[me], send_sem=dg_send_sem.at[k - 1], recv_sem=dg_recv_sem.at[k - 1], device_id=peer(k), device_id_type=pl.DeviceIdType.MESH)

    part_copies = [part_copy(k) for k in range(1, 16)]
    for c in part_copies:
        c.start()
    mi_copy.wait()
    lane_t = lax.broadcasted_iota(jnp.int32, (tokens, LANES), 1)
    mine = lane_t // half == t
    mean_ref[...] = jnp.where(mine, mean_ref[...], mi_recv[0])
    inv_ref[...] = jnp.where(mine, inv_ref[...], mi_recv[1])
    for c in fourth:
        c.wait_recv()
    flush = pltpu.make_async_copy(pool, pool_out, out_sem)
    flush.start()
    for c in part_copies:
        c.wait()
    dgb_ref[...] = jnp.sum(part_all[...], axis=0)
    for c in first[0] + first[1] + second[0] + second[1] + third[0] + third[1] + fourth:
        c.wait_send()
    flush.wait()


def front_call(feats, w_head, b_head, ln_gamma, ln_beta, labels, n_data):
    rows, tokens, width = feats.shape
    shard_cols = w_head.shape[1]
    n_w = shard_cols // WCOLS
    f32 = jnp.float32
    vmem = pl.BlockSpec(memory_space=pltpu.VMEM)
    anym = pl.BlockSpec(memory_space=pl.ANY)
    stat = jax.ShapeDtypeStruct((tokens, LANES), f32)
    return pl.pallas_call(
        front_kernel,
        name="front",
        in_specs=[anym, anym, vmem, vmem, vmem, vmem],
        out_specs=[anym, vmem, vmem, vmem, vmem, vmem, vmem],
        out_shape=[
            jax.ShapeDtypeStruct((rows * n_data, width), f32),
            stat,
            stat,
            jax.ShapeDtypeStruct((rows, width), f32),
            jax.ShapeDtypeStruct((8, LANES), f32),
            jax.ShapeDtypeStruct((8, LANES), f32),
            jax.ShapeDtypeStruct((2, width), f32),
        ],
        scratch_shapes=[
            pltpu.VMEM((SLOTS, GROUP, tokens, width), jnp.bfloat16),
            pltpu.VMEM((n_w, width, WCOLS), jnp.bfloat16),
            pltpu.VMEM((rows * n_data, width), f32),
            pltpu.VMEM((n_w, rows, WCOLS), f32),
            pltpu.VMEM((rows, width), jnp.bfloat16),
            pltpu.VMEM((8, LANES), f32),
            pltpu.VMEM((16, 8, LANES), f32),
            pltpu.VMEM((2, width), f32),
            pltpu.VMEM((16, 2, width), f32),
            pltpu.VMEM((2, tokens, LANES), f32),
            pltpu.VMEM((2, tokens, LANES), f32),
            pltpu.SemaphoreType.DMA((SLOTS,)),
            pltpu.SemaphoreType.DMA((n_w,)),
            pltpu.SemaphoreType.DMA((19,)),
            pltpu.SemaphoreType.DMA((19,)),
            pltpu.SemaphoreType.DMA((15,)),
            pltpu.SemaphoreType.DMA((15,)),
            pltpu.SemaphoreType.DMA((15,)),
            pltpu.SemaphoreType.DMA((15,)),
            pltpu.SemaphoreType.DMA,
        ],
        compiler_params=pltpu.CompilerParams(collective_id=0, has_side_effects=True, vmem_limit_bytes=63 * 2**20),
    )(feats, w_head, b_head.reshape(n_w, 1, WCOLS), ln_gamma[None, :], ln_beta[None, :], jnp.broadcast_to(labels[:, None], (rows, LANES)))


def head_kernel(shard_cols, pool_ref, gamma_ref, beta_ref, lse_ref, y_ref, w_ref, b_ref, dw_ref, db_ref, p_ref, pt_ref, lse_b, y_b, dl_ref):
    block = pl.program_id(0)
    rows, width = p_ref.shape

    @pl.when(block == 0)
    def _():
        def fill(r, carry):
            sl = pl.ds(r * LANES, LANES)
            p = pool_ref[sl, :] * gamma_ref[...] + beta_ref[...]
            p_ref[sl, :] = p.astype(jnp.bfloat16)
            lse_b[sl, :] = spread_row(lse_ref[pl.ds(r, 1), :])
            y_b[sl, :] = spread_row(y_ref[pl.ds(r, 1), :])
            return carry

        lax.fori_loop(0, rows // LANES, fill, 0)
        for r in range(rows // LANES):
            pt_ref[:, r * LANES:(r + 1) * LANES] = p_ref[r * LANES:(r + 1) * LANES, :].T

    base = lax.axis_index("tp") * shard_cols + block * COLS
    for s in range(COLS // SUB):
        sub = pl.ds(s * SUB, SUB)
        logits = jnp.dot(p_ref[...], w_ref[:, sub], preferred_element_type=jnp.float32)
        col = base + s * SUB + lax.broadcasted_iota(jnp.int32, (1, SUB), 1)
        valid = col < VALID_CLASSES
        smooth = jnp.where(valid, SMOOTH / VALID_CLASSES, 0.0)
        target = smooth + (1.0 - SMOOTH)
        bias = jnp.where(valid, b_ref[:, sub], -jnp.inf)
        soft = jnp.exp((logits + bias) - repeat_lanes(lse_b[...], SUB))
        dlogit = (soft - jnp.where(repeat_lanes(y_b[...], SUB) == col, target, smooth)) * (1.0 / rows)
        db_ref[:, sub] = jnp.sum(dlogit, axis=0, keepdims=True)
        dl_ref[s] = dlogit.astype(jnp.bfloat16)
    for s in range(COLS // SUB):
        dw_ref[:, pl.ds(s * SUB, SUB)] = jnp.dot(pt_ref[...], dl_ref[s], preferred_element_type=jnp.float32)


def resident(shape):
    return pl.BlockSpec(shape, lambda g: (0,) * len(shape), pipeline_mode=pl.Buffered(1))


def head_call(pool, ln_gamma, ln_beta, lse_all, y_all, w_head, b_head):
    rows, width = pool.shape
    shard_cols = w_head.shape[1]
    steps = shard_cols // COLS
    dw, db = pl.pallas_call(
        functools.partial(head_kernel, shard_cols),
        name="head",
        grid=(steps,),
        in_specs=[
            resident((rows, width)),
            resident((1, width)),
            resident((1, width)),
            resident((8, LANES)),
            resident((8, LANES)),
            pl.BlockSpec((width, COLS), lambda g: (0, g)),
            pl.BlockSpec((1, COLS), lambda g: (0, g)),
        ],
        out_specs=[pl.BlockSpec((width, COLS), lambda g: (0, g)), pl.BlockSpec((1, COLS), lambda g: (0, g))],
        out_shape=[jax.ShapeDtypeStruct((width, shard_cols), jnp.float32), jax.ShapeDtypeStruct((1, shard_cols), jnp.float32)],
        scratch_shapes=[
            pltpu.VMEM((rows, width), jnp.bfloat16),
            pltpu.VMEM((width, rows), jnp.bfloat16),
            pltpu.VMEM((rows, LANES), jnp.float32),
            pltpu.VMEM((rows, LANES), jnp.int32),
            pltpu.VMEM((COLS // SUB, rows, SUB), jnp.bfloat16),
        ],
        compiler_params=pltpu.CompilerParams(vmem_limit_bytes=48 * 2**20),
        cost_estimate=pl.CostEstimate(flops=4 * rows * width * shard_cols, bytes_accessed=6 * width * shard_cols, transcendentals=rows * shard_cols),
    )(pool, ln_gamma[None, :], ln_beta[None, :], lse_all, y_all, w_head, b_head[None, :])
    return dw, db[0]


def feat_kernel(x_ref, mean_ref, inv_ref, own_ref, other_ref, gamma_ref, df_ref):
    imgs, tokens, width = x_ref.shape
    chunks = tokens // ROW_TILE
    turn = (LANES - pl.program_id(0) * IMGS) % LANES
    u_all = (own_ref[...] + other_ref[...]) * gamma_ref[...] * (1.0 / tokens)
    us_all = jnp.sum(u_all, axis=1, keepdims=True)
    for i in range(imgs):
        u = u_all[i:i + 1, :]
        us = us_all[i:i + 1, :]
        um = us * (1.0 / width)
        for c in range(chunks):
            rows = pl.ds(c * ROW_TILE, ROW_TILE)
            mean = pltpu.roll(mean_ref[rows, :], turn, axis=1)[:, i:i + 1]
            inv = pltpu.roll(inv_ref[rows, :], turn, axis=1)[:, i:i + 1]
            x = x_ref[i, rows, :].astype(jnp.float32)
            proj = (jnp.sum(x * u, axis=1, keepdims=True) - mean * us) * (inv * (1.0 / width))
            slope = -(inv * inv * proj)
            offset = -(inv * um) - slope * mean
            x = x_ref[i, rows, :].astype(jnp.float32)
            df_ref[i, rows, :] = (x * slope + (u * inv + offset)).astype(jnp.bfloat16)


def feat_call(feats, mean, inv, own, other, ln_gamma):
    rows, tokens, width = feats.shape
    img = lambda shape: pl.BlockSpec(shape, lambda g: (g,) + (0,) * (len(shape) - 1))
    return pl.pallas_call(
        feat_kernel,
        name="feat",
        grid=(rows // IMGS,),
        in_specs=[img((IMGS, tokens, width)), resident((tokens, LANES)), resident((tokens, LANES)), img((IMGS, width)), img((IMGS, width)), resident((1, width))],
        out_specs=img((IMGS, tokens, width)),
        out_shape=jax.ShapeDtypeStruct(feats.shape, jnp.bfloat16),
        compiler_params=pltpu.CompilerParams(vmem_limit_bytes=48 * 2**20),
        cost_estimate=pl.CostEstimate(flops=10 * rows * tokens * width, bytes_accessed=4 * rows * tokens * width, transcendentals=0),
    )(feats, mean, inv, own, other, ln_gamma[None, :])


def solution(mesh):
    n_data = mesh.shape["dp"]

    def local_head(feats, ln_gamma, ln_beta, w_head, b_head, labels):
        rows = feats.shape[0]
        y_all = lax.all_gather(labels, "dp", axis=0, tiled=False)
        pool, mean, inv, dpool, lse_all, loss, dgb = front_call(feats, w_head, b_head, ln_gamma, ln_beta, labels, n_data)
        dpool_other = lax.ppermute(dpool, "tp", [(0, 1), (1, 0)])
        dw, db = head_call(pool, ln_gamma, ln_beta, lse_all, y_all, w_head, b_head)
        df = feat_call(feats, mean, inv, dpool, dpool_other, ln_gamma)
        return jnp.sum(loss[0]) / (rows * n_data), df, dw, db, dgb[0], dgb[1]

    return jax.shard_map(local_head, mesh=mesh, in_specs=(P("dp", None, None), P(), P(), P(None, "tp"), P("tp"), P("dp")), out_specs=(P(), P("dp", None, None), P(None, "tp"), P("tp"), P(), P()), check_vma=False)
```

```python
import functools
import math

import jax
import jax.numpy as jnp
from jax import lax
from jax.experimental import pallas as pl
from jax.experimental.pallas import tpu as pltpu
from jax.sharding import PartitionSpec as P

VALID_CLASSES = 21841
LN_EPS = 1e-5
SMOOTH = 0.1
LANES = 128
COLS = 1024
SUB = 256
IMGS = 8
ROW_TILE = 16
GROUP = 4
WCOLS = 1024
SLOTS = 3
PIECES = 4


def repeat_lanes(tile, width):
    return jnp.concatenate([tile] * (width // LANES), axis=1)


def fold_lanes(x, op):
    tiles = [x[:, j * LANES:(j + 1) * LANES] for j in range(x.shape[1] // LANES)]
    return functools.reduce(op, tiles)


def spread_row(row):
    return jnp.broadcast_to(row, (LANES, LANES)).T


def norm_image(x_ref, slot, i, lane_id, pool_row, pool_ref, mean_ref, inv_ref):
    _, _, tokens, width = x_ref.shape
    chunks = tokens // ROW_TILE
    lane = lax.broadcasted_iota(jnp.int32, (ROW_TILE, LANES), 1)
    means, invs = [], []
    for c in range(chunks):
        x = x_ref[slot, i, pl.ds(c * ROW_TILE, ROW_TILE), :].astype(jnp.float32)
        means.append(jnp.sum(x, axis=1, keepdims=True) * (1.0 / width))
    for c in range(chunks):
        x = x_ref[slot, i, pl.ds(c * ROW_TILE, ROW_TILE), :].astype(jnp.float32) - means[c]
        var = jnp.sum(x * x, axis=1, keepdims=True) * (1.0 / width)
        invs.append(lax.rsqrt(var + LN_EPS))
    total = jnp.zeros((ROW_TILE, width), jnp.float32)
    shift = jnp.zeros((ROW_TILE, 1), jnp.float32)
    for c in range(chunks):
        x = x_ref[slot, i, pl.ds(c * ROW_TILE, ROW_TILE), :].astype(jnp.float32)
        total = total + x * invs[c]
        shift = shift + means[c] * invs[c]
        rows = pl.ds(c * ROW_TILE, ROW_TILE)
        mean_ref[rows, :] = jnp.where(lane == lane_id, means[c], mean_ref[rows, :])
        inv_ref[rows, :] = jnp.where(lane == lane_id, invs[c], inv_ref[rows, :])
    pool_ref[pl.ds(pool_row, 1), :] = jnp.sum(total - shift, axis=0, keepdims=True) * (1.0 / tokens)


def front_kernel(x_hbm, w_hbm, b_ref, gamma_ref, beta_ref, y_ref,
                 pool_out, mean_ref, inv_ref, dpool_ref, lse_ref, yf_ref, loss_ref, dgamma_ref, dbeta_ref,
                 x_buf, w_buf, pool, logits, p16, stat_send, stat_recv, part, part_all, mi_send, mi_recv,
                 x_sem, w_sem, send_sem, recv_sem, st_send_sem, st_recv_sem, dg_send_sem, dg_recv_sem, out_sem):
    rows, tokens, width = x_hbm.shape
    half = rows // 2
    quarter = half // PIECES
    shard_cols = w_hbm.shape[1]
    n_w = shard_cols // WCOLS
    groups = half // GROUP
    rows_total = pool.shape[0]
    t = lax.axis_index("tp")
    d = lax.axis_index("dp")
    me = t * 8 + d
    dx = d + 2 - 4 * ((d // 2) % 2)
    dy = d + 4 - 8 * (d // 4)
    dxy = dx + 4 - 8 * (d // 4)

    def sibling(q):
        return q + 1 - 2 * (q % 2)

    def peer(k):
        q = (me + k) % 16
        return {"tp": q // 8, "dp": q % 8}

    barrier = pltpu.get_barrier_semaphore()
    for k in range(1, 16):
        pl.semaphore_signal(barrier, inc=1, device_id=peer(k), device_id_type=pl.DeviceIdType.MESH)

    def x_copy(g, slot):
        return pltpu.make_async_copy(x_hbm.at[pl.ds(t * half + g * GROUP, GROUP)], x_buf.at[slot], x_sem.at[slot])

    def w_copy(k):
        return pltpu.make_async_copy(w_hbm.at[:, pl.ds(k * WCOLS, WCOLS)], w_buf.at[k], w_sem.at[k])

    def chunk(q, tt, h):
        return pool.at[pl.ds(q * rows + tt * half + h * quarter, quarter)]

    def remote(ref, sem, target):
        return pltpu.make_async_remote_copy(src_ref=ref, dst_ref=ref, send_sem=send_sem.at[sem], recv_sem=recv_sem.at[sem], device_id=target, device_id_type=pl.DeviceIdType.MESH)

    to_z = {"tp": 1 - t, "dp": d}
    to_x = {"tp": t, "dp": dx}
    to_y = {"tp": t, "dp": dy}
    to_c = {"tp": t, "dp": sibling(d)}

    x_copy(0, 0).start()
    x_copy(1, 1).start()
    mean_ref[...] = jnp.zeros_like(mean_ref)
    inv_ref[...] = jnp.zeros_like(inv_ref)

    def do_group(g, carry):
        slot = g % SLOTS
        x_copy(g, slot).wait()

        @pl.when(g + 2 < groups)
        def _():
            x_copy(g + 2, (g + 2) % SLOTS).start()

        @pl.when(g % 3 != 2)
        def _():
            w_copy(g - g // 3).start()

        def image(i, c):
            local = t * half + g * GROUP + i
            norm_image(x_buf, slot, i, local, d * rows + local, pool, mean_ref, inv_ref)
            return c

        lax.fori_loop(0, GROUP, image, 0)
        return carry

    first = [[remote(chunk(d, t, j), 3 * j + a, to) for a, to in enumerate((to_z, to_x, to_y))] for j in range(PIECES)]
    second = [[remote(chunk(d, 1 - t, j), 12 + 2 * j + a, to) for a, to in enumerate((to_x, to_y))] for j in range(PIECES)]
    third = [[remote(chunk(dx, t, j), 20 + 2 * j, to_y), remote(chunk(dy, 1 - t, j), 21 + 2 * j, to_x)] for j in range(PIECES)]

    def block(q):
        return pool.at[pl.ds(q * rows, rows)]

    fourth = [remote(block(q), 28 + j, to_c) for j, q in enumerate((d, dx, dy, dxy))]
    mi_copy = pltpu.make_async_remote_copy(src_ref=mi_send, dst_ref=mi_recv, send_sem=send_sem.at[32], recv_sem=recv_sem.at[32], device_id=to_z, device_id_type=pl.DeviceIdType.MESH)

    def flush(j, q):
        return pltpu.make_async_copy(block(q), pool_out.at[pl.ds(q * rows, rows)], out_sem.at[j])

    flushes = [flush(j, q) for j, q in enumerate((d, dx, dy, dxy, sibling(d), sibling(dx), sibling(dy), sibling(dxy)))]

    def pass_z(j):
        first[j][0].wait_recv()
        for c in second[j]:
            c.start()

    def pass_x(j):
        first[j][1].wait_recv()
        third[j][0].start()

    def pass_y(j):
        second[j][1].wait_recv()
        third[j][1].start()

    for j in range(PIECES):
        lax.fori_loop(j * groups // PIECES, (j + 1) * groups // PIECES, do_group, 0)
        if j == 0:
            pl.semaphore_wait(barrier, 15)
        if j == PIECES - 1:
            mi_send[0] = mean_ref[...]
            mi_send[1] = inv_ref[...]
        for c in first[j]:
            c.start()
        if j >= 1:
            pass_z(j - 1)
            pass_x(j - 1)
        if j >= 2:
            pass_y(j - 2)
    pass_z(PIECES - 1)
    fourth[0].start()
    gamma = gamma_ref[...].reshape(1, width)
    beta = beta_ref[...].reshape(1, width)
    p16[...] = (pool[pl.ds(d * rows, rows), :] * gamma + beta).astype(jnp.bfloat16)

    def col_ids(k):
        return t * shard_cols + k * WCOLS + lax.broadcasted_iota(jnp.int32, (1, WCOLS), 1)

    def logits_step(k, top):
        w_copy(k).wait()
        cols = col_ids(k)
        bias = jnp.where(cols < VALID_CLASSES, b_ref[k], -jnp.inf)
        out = jnp.dot(p16[...], w_buf[k], preferred_element_type=jnp.float32) + bias
        logits[k] = out
        return jnp.maximum(top, fold_lanes(out, jnp.maximum))

    top = lax.fori_loop(0, n_w // 2, logits_step, jnp.full((rows, LANES), -jnp.inf, jnp.float32))
    mi_copy.start()
    pass_x(PIECES - 1)
    pass_y(PIECES - 2)
    top = lax.fori_loop(n_w // 2, n_w, logits_step, top)
    pass_y(PIECES - 1)
    for j in range(PIECES):
        second[j][0].wait_recv()
        first[j][2].wait_recv()
    fourth[1].start()
    fourth[2].start()
    row_top = jnp.broadcast_to(jnp.max(top, axis=1, keepdims=True), (rows, LANES))
    labels_f = spread_row(y_ref[...].astype(jnp.float32))
    labels = labels_f.astype(jnp.int32)
    zero = jnp.zeros((rows, LANES), jnp.float32)

    def stat_step(k, carry):
        total, target, valid_sum = carry
        cols = col_ids(k)
        out = logits[k]
        e = jnp.exp(out - repeat_lanes(row_top, WCOLS))
        hit = jnp.where(repeat_lanes(labels, WCOLS) == cols, out, 0.0)
        ok = jnp.where(cols < VALID_CLASSES, out, 0.0)
        return total + fold_lanes(e, jnp.add), target + fold_lanes(hit, jnp.add), valid_sum + fold_lanes(ok, jnp.add)

    total, target, valid_sum = lax.fori_loop(0, n_w, stat_step, (zero, zero, zero))
    lane = lax.broadcasted_iota(jnp.int32, (rows, LANES), 1)
    packed = jnp.where(lane == 0, row_top, jnp.where(lane == 1, jnp.sum(total, axis=1, keepdims=True), jnp.where(lane == 2, jnp.sum(target, axis=1, keepdims=True), jnp.where(lane == 3, jnp.sum(valid_sum, axis=1, keepdims=True), labels_f))))
    stat_send[...] = packed.T[:8]
    stat_recv[me] = stat_send[...]

    def stat_copy(k):
        return pltpu.make_async_remote_copy(src_ref=stat_send, dst_ref=stat_recv.at[me], send_sem=st_send_sem.at[k - 1], recv_sem=st_recv_sem.at[k - 1], device_id=peer(k), device_id_type=pl.DeviceIdType.MESH)

    stat_copies = [stat_copy(k) for k in range(1, 16)]
    for c in stat_copies:
        c.start()
    for c in flushes[:3]:
        c.start()
    for c in stat_copies:
        c.wait()

    def lse_of(q):
        a, b = stat_recv[q], stat_recv[8 + q]
        hi = jnp.maximum(a[0:1], b[0:1])
        return hi + jnp.log(a[1:2] * jnp.exp(a[0:1] - hi) + b[1:2] * jnp.exp(b[0:1] - hi))

    loss = jnp.zeros((1, LANES), jnp.float32)
    for q in range(8):
        lse_q = lse_of(q)
        lse_ref[q:q + 1, :] = lse_q
        a, b = stat_recv[q], stat_recv[8 + q]
        yf_ref[q:q + 1, :] = a[4:5]
        loss = loss + lse_q - (1.0 - SMOOTH) * (a[2:3] + b[2:3]) - (SMOOTH / VALID_CLASSES) * (a[3:4] + b[3:4])
    loss_ref[...] = jnp.broadcast_to(jnp.sum(loss, axis=1, keepdims=True) * (1.0 / rows_total), loss_ref.shape)
    lse_own = spread_row(lse_of(d))
    dpool_ref[...] = jnp.zeros_like(dpool_ref)

    def dpool_step(k, carry):
        cols = col_ids(k)
        smooth = jnp.where(cols < VALID_CLASSES, SMOOTH / VALID_CLASSES, 0.0)
        soft = jnp.exp(logits[k] - repeat_lanes(lse_own, WCOLS))
        dl = (soft - jnp.where(repeat_lanes(labels, WCOLS) == cols, smooth + (1.0 - SMOOTH), smooth)) * (1.0 / rows_total)
        dpool_ref[...] += lax.dot_general(dl.astype(jnp.bfloat16), w_buf[k], (((1,), (1,)), ((), ())), preferred_element_type=jnp.float32)
        return carry

    lax.fori_loop(0, n_w, dpool_step, 0)
    for j in range(PIECES):
        third[j][0].wait_recv()
        third[j][1].wait_recv()
    fourth[3].start()
    for c in fourth[:3]:
        c.wait_recv()
    for c in flushes[3:7]:
        c.start()
    dpool = dpool_ref[...]
    part[0:1, :] = jnp.sum(dpool * pool[pl.ds(d * rows, rows), :], axis=0, keepdims=True)
    part[1:2, :] = jnp.sum(dpool, axis=0, keepdims=True)
    part_all[me] = part[...]

    def part_copy(k):
        return pltpu.make_async_remote_copy(src_ref=part, dst_ref=part_all.at[me], send_sem=dg_send_sem.at[k - 1], recv_sem=dg_recv_sem.at[k - 1], device_id=peer(k), device_id_type=pl.DeviceIdType.MESH)

    part_copies = [part_copy(k) for k in range(1, 16)]
    for c in part_copies:
        c.start()
    mi_copy.wait()
    lane_t = lax.broadcasted_iota(jnp.int32, (tokens, LANES), 1)
    mine = lane_t // half == t
    mean_ref[...] = jnp.where(mine, mean_ref[...], mi_recv[0])
    inv_ref[...] = jnp.where(mine, inv_ref[...], mi_recv[1])
    fourth[3].wait_recv()
    flushes[7].start()
    for c in part_copies:
        c.wait()
    parts = jnp.sum(part_all[...], axis=0)
    dgamma_ref[...] = parts[0:1].reshape(width)
    dbeta_ref[...] = parts[1:2].reshape(width)
    for c in sum(first + second + third, []) + fourth:
        c.wait_send()
    for c in flushes:
        c.wait()


def front_call(feats, w_head, b_head, ln_gamma, ln_beta, labels, n_data):
    rows, tokens, width = feats.shape
    shard_cols = w_head.shape[1]
    n_w = shard_cols // WCOLS
    f32 = jnp.float32
    vmem = pl.BlockSpec(memory_space=pltpu.VMEM)
    anym = pl.BlockSpec(memory_space=pl.ANY)
    stat = jax.ShapeDtypeStruct((tokens, LANES), f32)
    return pl.pallas_call(
        front_kernel,
        name="front",
        in_specs=[anym, anym, vmem, vmem, vmem, vmem],
        out_specs=[anym] + [vmem] * 8,
        out_shape=[
            jax.ShapeDtypeStruct((rows * n_data, width), f32),
            stat,
            stat,
            jax.ShapeDtypeStruct((rows, width), f32),
            jax.ShapeDtypeStruct((8, LANES), f32),
            jax.ShapeDtypeStruct((8, LANES), f32),
            jax.ShapeDtypeStruct((8, LANES), f32),
            jax.ShapeDtypeStruct((width,), f32),
            jax.ShapeDtypeStruct((width,), f32),
        ],
        scratch_shapes=[
            pltpu.VMEM((SLOTS, GROUP, tokens, width), jnp.bfloat16),
            pltpu.VMEM((n_w, width, WCOLS), jnp.bfloat16),
            pltpu.VMEM((rows * n_data, width), f32),
            pltpu.VMEM((n_w, rows, WCOLS), f32),
            pltpu.VMEM((rows, width), jnp.bfloat16),
            pltpu.VMEM((8, LANES), f32),
            pltpu.VMEM((16, 8, LANES), f32),
            pltpu.VMEM((2, width), f32),
            pltpu.VMEM((16, 2, width), f32),
            pltpu.VMEM((2, tokens, LANES), f32),
            pltpu.VMEM((2, tokens, LANES), f32),
            pltpu.SemaphoreType.DMA((SLOTS,)),
            pltpu.SemaphoreType.DMA((n_w,)),
            pltpu.SemaphoreType.DMA((33,)),
            pltpu.SemaphoreType.DMA((33,)),
            pltpu.SemaphoreType.DMA((15,)),
            pltpu.SemaphoreType.DMA((15,)),
            pltpu.SemaphoreType.DMA((15,)),
            pltpu.SemaphoreType.DMA((15,)),
            pltpu.SemaphoreType.DMA((8,)),
        ],
        compiler_params=pltpu.CompilerParams(collective_id=0, has_side_effects=True, vmem_limit_bytes=63 * 2**20),
    )(feats, w_head, b_head.reshape(n_w, 1, WCOLS), ln_gamma, ln_beta, labels[None, :])


def head_kernel(shard_cols, pool_ref, gamma_ref, beta_ref, lse_ref, y_ref, w_ref, b_ref, dw_ref, db_ref, p_ref, pt_ref, lse_b, y_b, dl_ref):
    block = pl.program_id(0)
    rows, width = p_ref.shape

    @pl.when(block == 0)
    def _():
        def fill(r, carry):
            sl = pl.ds(r * LANES, LANES)
            p = pool_ref[sl, :] * gamma_ref[...].reshape(1, width) + beta_ref[...].reshape(1, width)
            p_ref[sl, :] = p.astype(jnp.bfloat16)
            lse_b[sl, :] = spread_row(lse_ref[pl.ds(r, 1), :])
            y_b[sl, :] = spread_row(y_ref[pl.ds(r, 1), :]).astype(jnp.int32)
            return carry

        lax.fori_loop(0, rows // LANES, fill, 0)
        for r in range(rows // LANES):
            pt_ref[:, r * LANES:(r + 1) * LANES] = p_ref[r * LANES:(r + 1) * LANES, :].T

    base = lax.axis_index("tp") * shard_cols + block * COLS
    n_sub = COLS // SUB

    def first_half(s):
        sub = pl.ds(s * SUB, SUB)
        logits = jnp.dot(p_ref[...], w_ref[:, sub], preferred_element_type=jnp.float32)
        col = base + s * SUB + lax.broadcasted_iota(jnp.int32, (1, SUB), 1)
        valid = col < VALID_CLASSES
        smooth = jnp.where(valid, SMOOTH / VALID_CLASSES, 0.0)
        target = smooth + (1.0 - SMOOTH)
        bias = jnp.where(valid, b_ref[:, sub], -jnp.inf)
        soft = jnp.exp((logits + bias) - repeat_lanes(lse_b[...], SUB))
        dlogit = (soft - jnp.where(repeat_lanes(y_b[...], SUB) == col, target, smooth)) * (1.0 / rows)
        db_ref[:, sub] = jnp.sum(dlogit, axis=0, keepdims=True)
        dl_ref[s] = dlogit.astype(jnp.bfloat16)

    def second_half(s):
        dw_ref[:, pl.ds(s * SUB, SUB)] = jnp.dot(pt_ref[...], dl_ref[s], preferred_element_type=jnp.float32)

    first_half(0)
    for s in range(1, n_sub):
        first_half(s)
        second_half(s - 1)
    second_half(n_sub - 1)


def resident(shape):
    return pl.BlockSpec(shape, lambda g: (0,) * len(shape), pipeline_mode=pl.Buffered(1))


def head_call(pool, ln_gamma, ln_beta, lse_all, y_all, w_head, b_head):
    rows, width = pool.shape
    shard_cols = w_head.shape[1]
    steps = shard_cols // COLS
    dw, db = pl.pallas_call(
        functools.partial(head_kernel, shard_cols),
        name="head",
        grid=(steps,),
        in_specs=[
            resident((rows, width)),
            resident((width,)),
            resident((width,)),
            resident((8, LANES)),
            resident((8, LANES)),
            pl.BlockSpec((width, COLS), lambda g: (0, g)),
            pl.BlockSpec((1, COLS), lambda g: (0, g)),
        ],
        out_specs=[pl.BlockSpec((width, COLS), lambda g: (0, g)), pl.BlockSpec((1, COLS), lambda g: (0, g))],
        out_shape=[jax.ShapeDtypeStruct((width, shard_cols), jnp.float32), jax.ShapeDtypeStruct((1, shard_cols), jnp.float32)],
        scratch_shapes=[
            pltpu.VMEM((rows, width), jnp.bfloat16),
            pltpu.VMEM((width, rows), jnp.bfloat16),
            pltpu.VMEM((rows, LANES), jnp.float32),
            pltpu.VMEM((rows, LANES), jnp.int32),
            pltpu.VMEM((COLS // SUB, rows, SUB), jnp.bfloat16),
        ],
        compiler_params=pltpu.CompilerParams(vmem_limit_bytes=56 * 2**20),
        cost_estimate=pl.CostEstimate(flops=4 * rows * width * shard_cols, bytes_accessed=6 * width * shard_cols, transcendentals=rows * shard_cols),
    )(pool, ln_gamma, ln_beta, lse_all, y_all, w_head, b_head[None, :])
    return dw, db[0]


def feat_kernel(x_ref, mean_ref, inv_ref, own_ref, other_ref, gamma_ref, df_ref, mean_t, inv_t):
    imgs, tokens, width = x_ref.shape
    chunks = tokens // ROW_TILE
    turn = (LANES - pl.program_id(0) * IMGS) % LANES
    mean_t[...] = pltpu.roll(mean_ref[...], turn, axis=1)
    inv_t[...] = pltpu.roll(inv_ref[...], turn, axis=1)
    u_all = (own_ref[...] + other_ref[...]) * gamma_ref[...].reshape(1, width) * (1.0 / tokens)
    us_all = jnp.sum(u_all, axis=1, keepdims=True) * (1.0 / width)
    for i in range(imgs):
        u = u_all[i:i + 1, :]
        um = jnp.broadcast_to(us_all[i:i + 1, :], (ROW_TILE, LANES))
        for c in range(chunks):
            rows = pl.ds(c * ROW_TILE, ROW_TILE)
            mean = jnp.broadcast_to(mean_t[rows, i:i + 1], (ROW_TILE, LANES))
            inv = jnp.broadcast_to(inv_t[rows, i:i + 1], (ROW_TILE, LANES))
            x = x_ref[i, rows, :].astype(jnp.float32)
            dots = jnp.broadcast_to(jnp.sum(x * u, axis=1, keepdims=True), (ROW_TILE, LANES))
            slope = -(inv * inv * inv) * (dots * (1.0 / width) - mean * um)
            offset = -(inv * um) - slope * mean
            x = x_ref[i, rows, :].astype(jnp.float32)
            df_ref[i, rows, :] = (x * repeat_lanes(slope, width) + (u * repeat_lanes(inv, width) + repeat_lanes(offset, width))).astype(jnp.bfloat16)


def feat_call(feats, mean, inv, own, other, ln_gamma):
    rows, tokens, width = feats.shape
    img = lambda shape: pl.BlockSpec(shape, lambda g: (g,) + (0,) * (len(shape) - 1))
    return pl.pallas_call(
        feat_kernel,
        name="feat",
        grid=(rows // IMGS,),
        in_specs=[img((IMGS, tokens, width)), resident((tokens, LANES)), resident((tokens, LANES)), img((IMGS, width)), img((IMGS, width)), resident((width,))],
        out_specs=img((IMGS, tokens, width)),
        scratch_shapes=[pltpu.VMEM((tokens, LANES), jnp.float32)] * 2,
        out_shape=jax.ShapeDtypeStruct(feats.shape, jnp.bfloat16),
        compiler_params=pltpu.CompilerParams(vmem_limit_bytes=48 * 2**20),
        cost_estimate=pl.CostEstimate(flops=10 * rows * tokens * width, bytes_accessed=4 * rows * tokens * width, transcendentals=0),
    )(feats, mean, inv, own, other, ln_gamma)


def solution(mesh):
    n_data = mesh.shape["dp"]

    def local_head(feats, ln_gamma, ln_beta, w_head, b_head, labels):
        pool, mean, inv, dpool, lse_all, y_all, loss, dgamma, dbeta = front_call(feats, w_head, b_head, ln_gamma, ln_beta, labels, n_data)
        dpool_other = lax.ppermute(dpool, "tp", [(0, 1), (1, 0)])
        dw, db = head_call(pool, ln_gamma, ln_beta, lse_all, y_all, w_head, b_head)
        df = feat_call(feats, mean, inv, dpool, dpool_other, ln_gamma)
        return loss[0, 0], df, dw, db, dgamma, dbeta

    return jax.shard_map(local_head, mesh=mesh, in_specs=(P("dp", None, None), P(), P(), P(None, "tp"), P("tp"), P("dp")), out_specs=(P(), P("dp", None, None), P(None, "tp"), P("tp"), P(), P()), check_vma=False)
```

```python
import functools
import math

import jax
import jax.numpy as jnp
from jax import lax
from jax.experimental import pallas as pl
from jax.experimental.pallas import tpu as pltpu
from jax.sharding import PartitionSpec as P

VALID_CLASSES = 21841
LN_EPS = 1e-5
SMOOTH = 0.1
LANES = 128
COLS = 512
SUB = 256
IMGS = 8
ROW_TILE = 16
GROUP = 4
WCOLS = 1024
SLOTS = 3
PIECES = 4
PARTS = 2


def repeat_lanes(tile, width):
    return jnp.concatenate([tile] * (width // LANES), axis=1)


def fold_lanes(x, op):
    tiles = [x[:, j * LANES:(j + 1) * LANES] for j in range(x.shape[1] // LANES)]
    return functools.reduce(op, tiles)


def spread_row(row):
    return jnp.broadcast_to(row, (LANES, LANES)).T


def norm_image(x_ref, slot, i, lane_id, pool_row, pool_ref, mean_ref, inv_ref):
    _, _, tokens, width = x_ref.shape
    chunks = tokens // ROW_TILE
    lane = lax.broadcasted_iota(jnp.int32, (ROW_TILE, LANES), 1)
    means, invs = [], []
    for c in range(chunks):
        x = x_ref[slot, i, pl.ds(c * ROW_TILE, ROW_TILE), :].astype(jnp.float32)
        means.append(jnp.sum(x, axis=1, keepdims=True) * (1.0 / width))
    for c in range(chunks):
        x = x_ref[slot, i, pl.ds(c * ROW_TILE, ROW_TILE), :].astype(jnp.float32) - means[c]
        var = jnp.sum(x * x, axis=1, keepdims=True) * (1.0 / width)
        invs.append(lax.rsqrt(var + LN_EPS))
    total = jnp.zeros((ROW_TILE, width), jnp.float32)
    shift = jnp.zeros((ROW_TILE, 1), jnp.float32)
    for c in range(chunks):
        x = x_ref[slot, i, pl.ds(c * ROW_TILE, ROW_TILE), :].astype(jnp.float32)
        total = total + x * invs[c]
        shift = shift + means[c] * invs[c]
        rows = pl.ds(c * ROW_TILE, ROW_TILE)
        mean_ref[rows, :] = jnp.where(lane == lane_id, means[c], mean_ref[rows, :])
        inv_ref[rows, :] = jnp.where(lane == lane_id, invs[c], inv_ref[rows, :])
    pool_ref[pl.ds(pool_row, 1), :] = jnp.sum(total - shift, axis=0, keepdims=True) * (1.0 / tokens)


def front_kernel(x_hbm, w_hbm, b_ref, gamma_ref, beta_ref, y_ref,
                 pool_out, mean_ref, inv_ref, dpool_ref, lse_ref, yf_ref, small_ref,
                 x_buf, w_buf, pool, logits, p16, stat_send, stat_recv, part, part_all, mi_send, mi_recv,
                 x_sem, w_sem, send_sem, recv_sem, st_send_sem, st_recv_sem, dg_send_sem, dg_recv_sem, out_sem):
    rows, tokens, width = x_hbm.shape
    half = rows // 2
    quarter = half // PIECES
    shard_cols = w_hbm.shape[1]
    n_w = shard_cols // WCOLS
    groups = half // GROUP
    rows_total = pool.shape[0]
    t = lax.axis_index("tp")
    d = lax.axis_index("dp")
    me = t * 8 + d
    dx = d + 2 - 4 * ((d // 2) % 2)
    dy = d + 4 - 8 * (d // 4)
    dxy = dx + 4 - 8 * (d // 4)

    def sibling(q):
        return q + 1 - 2 * (q % 2)

    def peer(k):
        q = (me + k) % 16
        return {"tp": q // 8, "dp": q % 8}

    barrier = pltpu.get_barrier_semaphore()
    for k in range(1, 16):
        pl.semaphore_signal(barrier, inc=1, device_id=peer(k), device_id_type=pl.DeviceIdType.MESH)

    def x_copy(g, slot):
        return pltpu.make_async_copy(x_hbm.at[pl.ds(t * half + g * GROUP, GROUP)], x_buf.at[slot], x_sem.at[slot])

    def w_copy(k):
        return pltpu.make_async_copy(w_hbm.at[:, pl.ds(k * WCOLS, WCOLS)], w_buf.at[k], w_sem.at[k])

    def chunk(q, tt, h):
        return pool.at[pl.ds(q * rows + tt * half + h * quarter, quarter)]

    def remote(ref, sem, target):
        return pltpu.make_async_remote_copy(src_ref=ref, dst_ref=ref, send_sem=send_sem.at[sem], recv_sem=recv_sem.at[sem], device_id=target, device_id_type=pl.DeviceIdType.MESH)

    to_z = {"tp": 1 - t, "dp": d}
    to_x = {"tp": t, "dp": dx}
    to_y = {"tp": t, "dp": dy}
    to_c = {"tp": t, "dp": sibling(d)}

    x_copy(0, 0).start()
    x_copy(1, 1).start()
    mean_ref[...] = jnp.zeros_like(mean_ref)
    inv_ref[...] = jnp.zeros_like(inv_ref)

    def do_group(g, carry):
        slot = g % SLOTS
        x_copy(g, slot).wait()

        @pl.when(g + 2 < groups)
        def _():
            x_copy(g + 2, (g + 2) % SLOTS).start()

        @pl.when(g % 3 != 2)
        def _():
            w_copy(g - g // 3).start()

        def image(i, c):
            local = t * half + g * GROUP + i
            norm_image(x_buf, slot, i, local, d * rows + local, pool, mean_ref, inv_ref)
            return c

        lax.fori_loop(0, GROUP, image, 0)
        return carry

    first = [[remote(chunk(d, t, j), 3 * j + a, to) for a, to in enumerate((to_z, to_x, to_y))] for j in range(PIECES)]
    second = [[remote(chunk(d, 1 - t, j), 12 + 2 * j + a, to) for a, to in enumerate((to_x, to_y))] for j in range(PIECES)]
    third = [[remote(chunk(dx, t, j), 20 + 2 * j, to_y), remote(chunk(dy, 1 - t, j), 21 + 2 * j, to_x)] for j in range(PIECES)]

    def block(q):
        return pool.at[pl.ds(q * rows, rows)]

    fourth = [remote(block(q), 28 + j, to_c) for j, q in enumerate((d, dx, dy, dxy))]
    mi_copy = pltpu.make_async_remote_copy(src_ref=mi_send, dst_ref=mi_recv, send_sem=send_sem.at[32], recv_sem=recv_sem.at[32], device_id=to_z, device_id_type=pl.DeviceIdType.MESH)

    def flush(j, q):
        return pltpu.make_async_copy(block(q), pool_out.at[pl.ds(q * rows, rows)], out_sem.at[j])

    flushes = [flush(j, q) for j, q in enumerate((d, dx, dy, dxy, sibling(d), sibling(dx), sibling(dy), sibling(dxy)))]

    def pass_z(j):
        first[j][0].wait_recv()
        for c in second[j]:
            c.start()

    def pass_x(j):
        first[j][1].wait_recv()
        third[j][0].start()

    def pass_y(j):
        second[j][1].wait_recv()
        third[j][1].start()

    for j in range(PIECES):
        lax.fori_loop(j * groups // PIECES, (j + 1) * groups // PIECES, do_group, 0)
        if j == 0:
            pl.semaphore_wait(barrier, 15)
        if j == PIECES - 1:
            mi_send[0] = mean_ref[...]
            mi_send[1] = inv_ref[...]
        for c in first[j]:
            c.start()
        if j >= 1:
            pass_z(j - 1)
            pass_x(j - 1)
        if j >= 2:
            pass_y(j - 2)
    pass_z(PIECES - 1)
    fourth[0].start()
    gamma = gamma_ref[...].reshape(1, width)
    beta = beta_ref[...].reshape(1, width)
    p16[...] = (pool[pl.ds(d * rows, rows), :] * gamma + beta).astype(jnp.bfloat16)

    def col_ids(k):
        return t * shard_cols + k * WCOLS + lax.broadcasted_iota(jnp.int32, (1, WCOLS), 1)

    def logits_step(k, top):
        w_copy(k).wait()
        cols = col_ids(k)
        bias = jnp.where(cols < VALID_CLASSES, b_ref[k], -jnp.inf)
        out = jnp.dot(p16[...], w_buf[k], preferred_element_type=jnp.float32) + bias
        logits[k] = out
        return jnp.maximum(top, fold_lanes(out, jnp.maximum))

    top = lax.fori_loop(0, n_w // 2, logits_step, jnp.full((rows, LANES), -jnp.inf, jnp.float32))
    mi_copy.start()
    pass_x(PIECES - 1)
    pass_y(PIECES - 2)
    top = lax.fori_loop(n_w // 2, n_w, logits_step, top)
    pass_y(PIECES - 1)
    for j in range(PIECES):
        second[j][0].wait_recv()
        first[j][2].wait_recv()
    fourth[1].start()
    fourth[2].start()
    row_top = jnp.broadcast_to(jnp.max(top, axis=1, keepdims=True), (rows, LANES))
    labels_f = spread_row(y_ref[...].astype(jnp.float32))
    labels = labels_f.astype(jnp.int32)
    zero = jnp.zeros((rows, LANES), jnp.float32)

    def stat_step(k, carry):
        total, target, valid_sum = carry
        cols = col_ids(k)
        out = logits[k]
        e = jnp.exp(out - repeat_lanes(row_top, WCOLS))
        hit = jnp.where(repeat_lanes(labels, WCOLS) == cols, out, 0.0)
        ok = jnp.where(cols < VALID_CLASSES, out, 0.0)
        return total + fold_lanes(e, jnp.add), target + fold_lanes(hit, jnp.add), valid_sum + fold_lanes(ok, jnp.add)

    total, target, valid_sum = lax.fori_loop(0, n_w, stat_step, (zero, zero, zero))
    lane = lax.broadcasted_iota(jnp.int32, (rows, LANES), 1)
    packed = jnp.where(lane == 0, row_top, jnp.where(lane == 1, jnp.sum(total, axis=1, keepdims=True), jnp.where(lane == 2, jnp.sum(target, axis=1, keepdims=True), jnp.where(lane == 3, jnp.sum(valid_sum, axis=1, keepdims=True), labels_f))))
    stat_send[...] = packed.T[:8]
    stat_recv[me] = stat_send[...]

    def stat_copy(k):
        return pltpu.make_async_remote_copy(src_ref=stat_send, dst_ref=stat_recv.at[me], send_sem=st_send_sem.at[k - 1], recv_sem=st_recv_sem.at[k - 1], device_id=peer(k), device_id_type=pl.DeviceIdType.MESH)

    stat_copies = [stat_copy(k) for k in range(1, 16)]
    for c in stat_copies:
        c.start()
    for c in flushes[:3]:
        c.start()
    for c in stat_copies:
        c.wait()

    def lse_of(q):
        a, b = stat_recv[q], stat_recv[8 + q]
        hi = jnp.maximum(a[0:1], b[0:1])
        return hi + jnp.log(a[1:2] * jnp.exp(a[0:1] - hi) + b[1:2] * jnp.exp(b[0:1] - hi))

    loss = jnp.zeros((1, LANES), jnp.float32)
    for q in range(8):
        lse_q = lse_of(q)
        lse_ref[q:q + 1, :] = lse_q
        a, b = stat_recv[q], stat_recv[8 + q]
        yf_ref[q:q + 1, :] = a[4:5]
        loss = loss + lse_q - (1.0 - SMOOTH) * (a[2:3] + b[2:3]) - (SMOOTH / VALID_CLASSES) * (a[3:4] + b[3:4])
    small_ref[2:3, :] = jnp.broadcast_to(jnp.sum(loss, axis=1, keepdims=True) * (1.0 / rows_total), (1, width))
    small_ref[3:8, :] = jnp.zeros((5, width), jnp.float32)
    lse_own = spread_row(lse_of(d))
    dpool_ref[...] = jnp.zeros_like(dpool_ref)

    def dpool_step(k, carry):
        cols = col_ids(k)
        smooth = jnp.where(cols < VALID_CLASSES, SMOOTH / VALID_CLASSES, 0.0)
        soft = jnp.exp(logits[k] - repeat_lanes(lse_own, WCOLS))
        dl = (soft - jnp.where(repeat_lanes(labels, WCOLS) == cols, smooth + (1.0 - SMOOTH), smooth)) * (1.0 / rows_total)
        dpool_ref[...] += lax.dot_general(dl.astype(jnp.bfloat16), w_buf[k], (((1,), (1,)), ((), ())), preferred_element_type=jnp.float32)
        return carry

    lax.fori_loop(0, n_w, dpool_step, 0)
    for j in range(PIECES):
        third[j][0].wait_recv()
        third[j][1].wait_recv()
    fourth[3].start()
    for c in fourth[:3]:
        c.wait_recv()
    for c in flushes[3:7]:
        c.start()
    dpool = dpool_ref[...]
    part[0:1, :] = jnp.sum(dpool * pool[pl.ds(d * rows, rows), :], axis=0, keepdims=True)
    part[1:2, :] = jnp.sum(dpool, axis=0, keepdims=True)
    part_all[me] = part[...]

    def part_copy(k):
        return pltpu.make_async_remote_copy(src_ref=part, dst_ref=part_all.at[me], send_sem=dg_send_sem.at[k - 1], recv_sem=dg_recv_sem.at[k - 1], device_id=peer(k), device_id_type=pl.DeviceIdType.MESH)

    part_copies = [part_copy(k) for k in range(1, 16)]
    for c in part_copies:
        c.start()
    mi_copy.wait()
    lane_t = lax.broadcasted_iota(jnp.int32, (tokens, LANES), 1)
    mine = lane_t // half == t
    mean_ref[...] = jnp.where(mine, mean_ref[...], mi_recv[0])
    inv_ref[...] = jnp.where(mine, inv_ref[...], mi_recv[1])
    fourth[3].wait_recv()
    flushes[7].start()
    for c in part_copies:
        c.wait()
    small_ref[0:2, :] = jnp.sum(part_all[...], axis=0)
    for c in sum(first + second + third, []) + fourth:
        c.wait_send()
    for c in flushes:
        c.wait()


def front_call(feats, w_head, b_head, ln_gamma, ln_beta, labels, n_data):
    rows, tokens, width = feats.shape
    shard_cols = w_head.shape[1]
    n_w = shard_cols // WCOLS
    f32 = jnp.float32
    vmem = pl.BlockSpec(memory_space=pltpu.VMEM)
    anym = pl.BlockSpec(memory_space=pl.ANY)
    stat = jax.ShapeDtypeStruct((tokens, LANES), f32)
    return pl.pallas_call(
        front_kernel,
        name="front",
        in_specs=[anym, anym, vmem, vmem, vmem, vmem],
        out_specs=[anym] + [vmem] * 6,
        out_shape=[
            jax.ShapeDtypeStruct((rows * n_data, width), f32),
            stat,
            stat,
            jax.ShapeDtypeStruct((rows, width), f32),
            jax.ShapeDtypeStruct((8, LANES), f32),
            jax.ShapeDtypeStruct((8, LANES), f32),
            jax.ShapeDtypeStruct((8, width), f32),
        ],
        scratch_shapes=[
            pltpu.VMEM((SLOTS, GROUP, tokens, width), jnp.bfloat16),
            pltpu.VMEM((n_w, width, WCOLS), jnp.bfloat16),
            pltpu.VMEM((rows * n_data, width), f32),
            pltpu.VMEM((n_w, rows, WCOLS), f32),
            pltpu.VMEM((rows, width), jnp.bfloat16),
            pltpu.VMEM((8, LANES), f32),
            pltpu.VMEM((16, 8, LANES), f32),
            pltpu.VMEM((2, width), f32),
            pltpu.VMEM((16, 2, width), f32),
            pltpu.VMEM((2, tokens, LANES), f32),
            pltpu.VMEM((2, tokens, LANES), f32),
            pltpu.SemaphoreType.DMA((SLOTS,)),
            pltpu.SemaphoreType.DMA((n_w,)),
            pltpu.SemaphoreType.DMA((33,)),
            pltpu.SemaphoreType.DMA((33,)),
            pltpu.SemaphoreType.DMA((15,)),
            pltpu.SemaphoreType.DMA((15,)),
            pltpu.SemaphoreType.DMA((15,)),
            pltpu.SemaphoreType.DMA((15,)),
            pltpu.SemaphoreType.DMA((8,)),
        ],
        compiler_params=pltpu.CompilerParams(collective_id=0, has_side_effects=True, vmem_limit_bytes=63 * 2**20),
    )(feats, w_head, b_head.reshape(n_w, 1, WCOLS), ln_gamma, ln_beta, labels[None, :])


def fill_rows(pool_ref, gamma_ref, beta_ref, lse_ref, y_ref, p_ref, pt_ref, lse_b, y_b):
    rows, width = p_ref.shape

    @pl.when(pl.program_id(0) == 0)
    def _():
        def fill(r, carry):
            sl = pl.ds(r * LANES, LANES)
            p = pool_ref[sl, :] * gamma_ref[...].reshape(1, width) + beta_ref[...].reshape(1, width)
            p_ref[sl, :] = p.astype(jnp.bfloat16)
            lse_b[sl, :] = spread_row(lse_ref[pl.ds(r, 1), :] + math.log(rows))
            y_b[sl, :] = spread_row(y_ref[pl.ds(r, 1), :]).astype(jnp.int32)
            return carry

        lax.fori_loop(0, rows // LANES, fill, 0)
        for r in range(rows // LANES):
            pt_ref[:, r * LANES:(r + 1) * LANES] = p_ref[r * LANES:(r + 1) * LANES, :].T


def head_pieces(base, p_ref, pt_ref, lse_b, y_b, w_ref, b_ref, dw_ref, db_ref, dl_ref, parts):
    rows, width = p_ref.shape

    def first_half(s, m):
        sub = pl.ds(s * SUB, SUB)
        part = pl.ds(m * (rows // parts), rows // parts)
        logits = jnp.dot(p_ref[part, :], w_ref[:, sub], preferred_element_type=jnp.float32)
        col = base + s * SUB + lax.broadcasted_iota(jnp.int32, (1, SUB), 1)
        valid = col < VALID_CLASSES
        smooth = jnp.where(valid, SMOOTH / VALID_CLASSES / rows, 0.0)
        target = smooth + (1.0 - SMOOTH) / rows
        bias = jnp.where(valid, b_ref[:, sub], -jnp.inf)
        soft = jnp.exp((logits + bias) - repeat_lanes(lse_b[part, :], SUB))
        dlogit = soft - jnp.where(repeat_lanes(y_b[part, :], SUB) == col, target, smooth)
        db = jnp.sum(dlogit, axis=0, keepdims=True)
        db_ref[:, sub] = db if m == 0 else db_ref[:, sub] + db
        dl_ref[s, part, :] = dlogit.astype(jnp.bfloat16)

    def second_half(s, m):
        part = pl.ds(m * (width // parts), width // parts)
        dw_ref[part, pl.ds(s * SUB, SUB)] = jnp.dot(pt_ref[part, :], dl_ref[s], preferred_element_type=jnp.float32)

    n_sub = COLS // SUB
    order = [functools.partial(first_half, 0, m) for m in range(parts)]
    for s in range(1, n_sub):
        order += [functools.partial(first_half, s, m) for m in range(parts)]
        order += [functools.partial(second_half, s - 1, m) for m in range(parts)]
    return order + [functools.partial(second_half, n_sub - 1, m) for m in range(parts)]


def head_kernel(shard_cols, pool_ref, gamma_ref, beta_ref, lse_ref, y_ref, w_ref, b_ref, dw_ref, db_ref, p_ref, pt_ref, lse_b, y_b, dl_ref):
    fill_rows(pool_ref, gamma_ref, beta_ref, lse_ref, y_ref, p_ref, pt_ref, lse_b, y_b)
    base = lax.axis_index("tp") * shard_cols + pl.program_id(0) * COLS
    for piece in head_pieces(base, p_ref, pt_ref, lse_b, y_b, w_ref, b_ref, dw_ref, db_ref, dl_ref, 1):
        piece()


def feat_image(i, x_ref, mean_t, inv_t, u_ref, df_ref):
    imgs, tokens, width = x_ref.shape
    u = u_ref[pl.ds(i, 1), :]
    um = jnp.broadcast_to(jnp.sum(u, axis=1, keepdims=True) * (1.0 / width), (ROW_TILE, LANES))
    for c in range(tokens // ROW_TILE):
        rows = pl.ds(c * ROW_TILE, ROW_TILE)
        mean = jnp.broadcast_to(mean_t[rows, i:i + 1], (ROW_TILE, LANES))
        inv = jnp.broadcast_to(inv_t[rows, i:i + 1], (ROW_TILE, LANES))
        x = x_ref[i, rows, :].astype(jnp.float32)
        dots = jnp.broadcast_to(jnp.sum(x * u, axis=1, keepdims=True), (ROW_TILE, LANES))
        slope = -(inv * inv * inv) * (dots * (1.0 / width) - mean * um)
        offset = -(inv * um) - slope * mean
        x = x_ref[i, rows, :].astype(jnp.float32)
        df_ref[i, rows, :] = (x * repeat_lanes(slope, width) + (u * repeat_lanes(inv, width) + repeat_lanes(offset, width))).astype(jnp.bfloat16)


def head_feat_kernel(shard_cols, first, pool_ref, gamma_ref, beta_ref, lse_ref, y_ref, w_ref, b_ref, x_ref, mean_ref, inv_ref, own_ref, other_ref, small_ref, dw_in, db_in,
                     dw_ref, db_ref, df_ref, small_out, p_ref, pt_ref, lse_b, y_b, dl_ref, mean_t, inv_t, u_ref):
    imgs, tokens, width = x_ref.shape
    fill_rows(pool_ref, gamma_ref, beta_ref, lse_ref, y_ref, p_ref, pt_ref, lse_b, y_b)
    small_out[...] = small_ref[...]
    turn = (LANES - pl.program_id(0) * imgs) % LANES
    mean_t[...] = pltpu.roll(mean_ref[...], turn, axis=1)
    inv_t[...] = pltpu.roll(inv_ref[...], turn, axis=1)
    u_ref[...] = (own_ref[...] + other_ref[...]) * gamma_ref[...].reshape(1, width) * (1.0 / tokens)
    base = lax.axis_index("tp") * shard_cols + (pl.program_id(0) + first) * COLS
    pieces = head_pieces(base, p_ref, pt_ref, lse_b, y_b, w_ref, b_ref, dw_ref, db_ref, dl_ref, PARTS)
    for n, piece in enumerate(pieces):
        piece()
        for i in range(n * imgs // len(pieces), (n + 1) * imgs // len(pieces)):
            feat_image(i, x_ref, mean_t, inv_t, u_ref, df_ref)


def resident(shape):
    return pl.BlockSpec(shape, lambda g: (0,) * len(shape), pipeline_mode=pl.Buffered(1))


def head_calls(pool, ln_gamma, ln_beta, lse_all, y_all, w_head, b_head, feats, mean, inv, own, make_other, small):
    rows, width = pool.shape
    shard_cols = w_head.shape[1]
    imgs_all, tokens, _ = feats.shape
    feat_steps = imgs_all // IMGS
    first = shard_cols // COLS - feat_steps
    f32 = jnp.float32
    args = (pool, ln_gamma, ln_beta, lse_all, y_all, w_head, b_head[None, :])
    dw_shape = jax.ShapeDtypeStruct((width, shard_cols), f32)
    db_shape = jax.ShapeDtypeStruct((1, shard_cols), f32)
    scratch = [
        pltpu.VMEM((rows, width), jnp.bfloat16),
        pltpu.VMEM((width, rows), jnp.bfloat16),
        pltpu.VMEM((rows, LANES), f32),
        pltpu.VMEM((rows, LANES), jnp.int32),
        pltpu.VMEM((COLS // SUB, rows, SUB), jnp.bfloat16),
    ]

    def specs(skip):
        return [
            resident((rows, width)),
            resident((width,)),
            resident((width,)),
            resident((8, LANES)),
            resident((8, LANES)),
            pl.BlockSpec((width, COLS), lambda g: (0, g + skip)),
            pl.BlockSpec((1, COLS), lambda g: (0, g + skip)),
        ]

    def outs(skip):
        return [pl.BlockSpec((width, COLS), lambda g: (0, g + skip)), pl.BlockSpec((1, COLS), lambda g: (0, g + skip))]

    def cost(n):
        return pl.CostEstimate(flops=4 * rows * width * COLS * n, bytes_accessed=6 * width * COLS * n, transcendentals=rows * COLS * n)

    params = pltpu.CompilerParams(vmem_limit_bytes=56 * 2**20)
    dw, db = pl.pallas_call(
        functools.partial(head_kernel, shard_cols),
        name="head",
        grid=(first,),
        in_specs=specs(0),
        out_specs=outs(0),
        out_shape=[dw_shape, db_shape],
        scratch_shapes=scratch,
        compiler_params=params,
        cost_estimate=cost(first),
    )(*args)
    other = make_other
    img = lambda shape: pl.BlockSpec(shape, lambda g: (g,) + (0,) * (len(shape) - 1))
    n_in = 13
    dw, db, df, small = pl.pallas_call(
        functools.partial(head_feat_kernel, shard_cols, first),
        name="head_feat",
        grid=(feat_steps,),
        in_specs=specs(first)
        + [img((IMGS, tokens, width)), resident((tokens, LANES)), resident((tokens, LANES)), img((IMGS, width)), img((IMGS, width)), resident(small.shape)]
        + [pl.BlockSpec(memory_space=pl.ANY)] * 2,
        out_specs=outs(first) + [img((IMGS, tokens, width)), pl.BlockSpec(small.shape, lambda g: (0, 0))],
        out_shape=[dw_shape, db_shape, jax.ShapeDtypeStruct(feats.shape, jnp.bfloat16), jax.ShapeDtypeStruct(small.shape, f32)],
        scratch_shapes=scratch + [pltpu.VMEM((tokens, LANES), f32)] * 2 + [pltpu.VMEM((IMGS, width), f32)],
        input_output_aliases={n_in: 0, n_in + 1: 1},
        compiler_params=params,
        cost_estimate=cost(feat_steps),
    )(*args, feats, mean, inv, own, other, small, dw, db)
    return dw, db[0], df, small


def solution(mesh):
    n_data = mesh.shape["dp"]

    def local_head(feats, ln_gamma, ln_beta, w_head, b_head, labels):
        pool, mean, inv, dpool, lse_all, y_all, small = front_call(feats, w_head, b_head, ln_gamma, ln_beta, labels, n_data)
        dpool_other = lax.ppermute(dpool, "tp", [(0, 1), (1, 0)])
        dw, db, df, small = head_calls(pool, ln_gamma, ln_beta, lse_all, y_all, w_head, b_head, feats, mean, inv, dpool, dpool_other, small)
        return small[2, 0], df, dw, db, small[0], small[1]

    return jax.shard_map(local_head, mesh=mesh, in_specs=(P("dp", None, None), P(), P(), P(None, "tp"), P("tp"), P("dp")), out_specs=(P(), P("dp", None, None), P(None, "tp"), P("tp"), P(), P()), check_vma=False)
```

```python
import functools
import math

import jax
import jax.numpy as jnp
from jax import lax
from jax.experimental import pallas as pl
from jax.experimental.pallas import tpu as pltpu
from jax.sharding import PartitionSpec as P

VALID_CLASSES = 21841
LN_EPS = 1e-5
SMOOTH = 0.1
LANES = 128
COLS = 512
LEAD_COLS = 1024
SUB = 256
IMGS = 8
ROW_TILE = 16
GROUP = 4
WCOLS = 1024
SLOTS = 3
PIECES = 4
PARTS = 2


def repeat_lanes(tile, width):
    return jnp.concatenate([tile] * (width // LANES), axis=1)


def fold_lanes(x, op):
    tiles = [x[:, j * LANES:(j + 1) * LANES] for j in range(x.shape[1] // LANES)]
    return functools.reduce(op, tiles)


def spread_row(row):
    return jnp.broadcast_to(row, (LANES, LANES)).T


def norm_image(x_ref, slot, i, lane_id, pool_row, pool_ref, mean_ref, inv_ref):
    _, _, tokens, width = x_ref.shape
    chunks = tokens // ROW_TILE
    lane = lax.broadcasted_iota(jnp.int32, (ROW_TILE, LANES), 1)
    means, invs = [], []
    for c in range(chunks):
        x = x_ref[slot, i, pl.ds(c * ROW_TILE, ROW_TILE), :].astype(jnp.float32)
        means.append(jnp.sum(x, axis=1, keepdims=True) * (1.0 / width))
    for c in range(chunks):
        x = x_ref[slot, i, pl.ds(c * ROW_TILE, ROW_TILE), :].astype(jnp.float32) - means[c]
        var = jnp.sum(x * x, axis=1, keepdims=True) * (1.0 / width)
        invs.append(lax.rsqrt(var + LN_EPS))
    total = jnp.zeros((ROW_TILE, width), jnp.float32)
    shift = jnp.zeros((ROW_TILE, 1), jnp.float32)
    for c in range(chunks):
        x = x_ref[slot, i, pl.ds(c * ROW_TILE, ROW_TILE), :].astype(jnp.float32)
        total = total + x * invs[c]
        shift = shift + means[c] * invs[c]
        rows = pl.ds(c * ROW_TILE, ROW_TILE)
        mean_ref[rows, :] = jnp.where(lane == lane_id, means[c], mean_ref[rows, :])
        inv_ref[rows, :] = jnp.where(lane == lane_id, invs[c], inv_ref[rows, :])
    pool_ref[pl.ds(pool_row, 1), :] = jnp.sum(total - shift, axis=0, keepdims=True) * (1.0 / tokens)


def front_kernel(x_hbm, w_hbm, b_ref, gamma_ref, beta_ref, y_ref,
                 pool_out, mean_ref, inv_ref, dpool_ref, lse_ref, yf_ref, small_ref,
                 x_buf, w_buf, pool, logits, p16, stat_send, stat_recv, part, part_all, mi_send, mi_recv,
                 x_sem, w_sem, send_sem, recv_sem, st_send_sem, st_recv_sem, dg_send_sem, dg_recv_sem, out_sem):
    rows, tokens, width = x_hbm.shape
    half = rows // 2
    quarter = half // PIECES
    shard_cols = w_hbm.shape[1]
    n_w = shard_cols // WCOLS
    groups = half // GROUP
    rows_total = pool.shape[0]
    t = lax.axis_index("tp")
    d = lax.axis_index("dp")
    me = t * 8 + d
    dx = d + 2 - 4 * ((d // 2) % 2)
    dy = d + 4 - 8 * (d // 4)
    dxy = dx + 4 - 8 * (d // 4)

    def sibling(q):
        return q + 1 - 2 * (q % 2)

    def peer(k):
        q = (me + k) % 16
        return {"tp": q // 8, "dp": q % 8}

    barrier = pltpu.get_barrier_semaphore()
    for k in range(1, 16):
        pl.semaphore_signal(barrier, inc=1, device_id=peer(k), device_id_type=pl.DeviceIdType.MESH)

    def x_copy(g, slot):
        return pltpu.make_async_copy(x_hbm.at[pl.ds(t * half + g * GROUP, GROUP)], x_buf.at[slot], x_sem.at[slot])

    def w_copy(k):
        return pltpu.make_async_copy(w_hbm.at[:, pl.ds(k * WCOLS, WCOLS)], w_buf.at[k], w_sem.at[k])

    def chunk(q, tt, h):
        return pool.at[pl.ds(q * rows + tt * half + h * quarter, quarter)]

    def remote(ref, sem, target):
        return pltpu.make_async_remote_copy(src_ref=ref, dst_ref=ref, send_sem=send_sem.at[sem], recv_sem=recv_sem.at[sem], device_id=target, device_id_type=pl.DeviceIdType.MESH)

    to_z = {"tp": 1 - t, "dp": d}
    to_x = {"tp": t, "dp": dx}
    to_y = {"tp": t, "dp": dy}
    to_c = {"tp": t, "dp": sibling(d)}

    x_copy(0, 0).start()
    x_copy(1, 1).start()
    mean_ref[...] = jnp.zeros_like(mean_ref)
    inv_ref[...] = jnp.zeros_like(inv_ref)

    def do_group(g, carry):
        slot = g % SLOTS
        x_copy(g, slot).wait()

        @pl.when(g + 2 < groups)
        def _():
            x_copy(g + 2, (g + 2) % SLOTS).start()

        @pl.when(g % 3 != 2)
        def _():
            w_copy(g - g // 3).start()

        def image(i, c):
            local = t * half + g * GROUP + i
            norm_image(x_buf, slot, i, local, d * rows + local, pool, mean_ref, inv_ref)
            return c

        lax.fori_loop(0, GROUP, image, 0)
        return carry

    first = [[remote(chunk(d, t, j), 3 * j + a, to) for a, to in enumerate((to_z, to_x, to_y))] for j in range(PIECES)]
    second = [[remote(chunk(d, 1 - t, j), 12 + 2 * j + a, to) for a, to in enumerate((to_x, to_y))] for j in range(PIECES)]
    third = [[remote(chunk(dx, t, j), 20 + 2 * j, to_y), remote(chunk(dy, 1 - t, j), 21 + 2 * j, to_x)] for j in range(PIECES)]

    def block(q):
        return pool.at[pl.ds(q * rows, rows)]

    fourth = [remote(block(q), 28 + j, to_c) for j, q in enumerate((d, dx, dy, dxy))]
    mi_copy = pltpu.make_async_remote_copy(src_ref=mi_send, dst_ref=mi_recv, send_sem=send_sem.at[32], recv_sem=recv_sem.at[32], device_id=to_z, device_id_type=pl.DeviceIdType.MESH)

    def flush(j, q):
        return pltpu.make_async_copy(block(q), pool_out.at[pl.ds(q * rows, rows)], out_sem.at[j])

    flushes = [flush(j, q) for j, q in enumerate((d, dx, dy, dxy, sibling(d), sibling(dx), sibling(dy), sibling(dxy)))]

    def pass_z(j):
        first[j][0].wait_recv()
        for c in second[j]:
            c.start()

    def pass_x(j):
        first[j][1].wait_recv()
        third[j][0].start()

    def pass_y(j):
        second[j][1].wait_recv()
        third[j][1].start()

    for j in range(PIECES):
        lax.fori_loop(j * groups // PIECES, (j + 1) * groups // PIECES, do_group, 0)
        if j == 0:
            pl.semaphore_wait(barrier, 15)
        if j == PIECES - 1:
            mi_send[0] = mean_ref[...]
            mi_send[1] = inv_ref[...]
        for c in first[j]:
            c.start()
        if j >= 1:
            pass_z(j - 1)
            pass_x(j - 1)
        if j >= 2:
            pass_y(j - 2)
    pass_z(PIECES - 1)
    fourth[0].start()
    gamma = gamma_ref[...].reshape(1, width)
    beta = beta_ref[...].reshape(1, width)
    p16[...] = (pool[pl.ds(d * rows, rows), :] * gamma + beta).astype(jnp.bfloat16)

    def col_ids(k):
        return t * shard_cols + k * WCOLS + lax.broadcasted_iota(jnp.int32, (1, WCOLS), 1)

    def logits_step(k, top):
        w_copy(k).wait()
        cols = col_ids(k)
        bias = jnp.where(cols < VALID_CLASSES, b_ref[k], -jnp.inf)
        out = jnp.dot(p16[...], w_buf[k], preferred_element_type=jnp.float32) + bias
        logits[k] = out
        return jnp.maximum(top, fold_lanes(out, jnp.maximum))

    top = lax.fori_loop(0, n_w // 2, logits_step, jnp.full((rows, LANES), -jnp.inf, jnp.float32))
    mi_copy.start()
    pass_x(PIECES - 1)
    pass_y(PIECES - 2)
    top = lax.fori_loop(n_w // 2, n_w, logits_step, top)
    pass_y(PIECES - 1)
    for j in range(PIECES):
        second[j][0].wait_recv()
        first[j][2].wait_recv()
    fourth[1].start()
    fourth[2].start()
    row_top = jnp.broadcast_to(jnp.max(top, axis=1, keepdims=True), (rows, LANES))
    labels_f = spread_row(y_ref[...].astype(jnp.float32))
    labels = labels_f.astype(jnp.int32)
    zero = jnp.zeros((rows, LANES), jnp.float32)

    def stat_step(k, carry):
        total, target, valid_sum = carry
        cols = col_ids(k)
        out = logits[k]
        e = jnp.exp(out - repeat_lanes(row_top, WCOLS))
        hit = jnp.where(repeat_lanes(labels, WCOLS) == cols, out, 0.0)
        ok = jnp.where(cols < VALID_CLASSES, out, 0.0)
        return total + fold_lanes(e, jnp.add), target + fold_lanes(hit, jnp.add), valid_sum + fold_lanes(ok, jnp.add)

    total, target, valid_sum = lax.fori_loop(0, n_w, stat_step, (zero, zero, zero))
    lane = lax.broadcasted_iota(jnp.int32, (rows, LANES), 1)
    packed = jnp.where(lane == 0, row_top, jnp.where(lane == 1, jnp.sum(total, axis=1, keepdims=True), jnp.where(lane == 2, jnp.sum(target, axis=1, keepdims=True), jnp.where(lane == 3, jnp.sum(valid_sum, axis=1, keepdims=True), labels_f))))
    stat_send[...] = packed.T[:8]
    stat_recv[me] = stat_send[...]

    def stat_copy(k):
        return pltpu.make_async_remote_copy(src_ref=stat_send, dst_ref=stat_recv.at[me], send_sem=st_send_sem.at[k - 1], recv_sem=st_recv_sem.at[k - 1], device_id=peer(k), device_id_type=pl.DeviceIdType.MESH)

    stat_copies = [stat_copy(k) for k in range(1, 16)]
    for c in stat_copies:
        c.start()
    for c in flushes[:3]:
        c.start()
    for c in stat_copies:
        c.wait()

    def lse_of(q):
        a, b = stat_recv[q], stat_recv[8 + q]
        hi = jnp.maximum(a[0:1], b[0:1])
        return hi + jnp.log(a[1:2] * jnp.exp(a[0:1] - hi) + b[1:2] * jnp.exp(b[0:1] - hi))

    loss = jnp.zeros((1, LANES), jnp.float32)
    for q in range(8):
        lse_q = lse_of(q)
        lse_ref[q:q + 1, :] = lse_q
        a, b = stat_recv[q], stat_recv[8 + q]
        yf_ref[q:q + 1, :] = a[4:5]
        loss = loss + lse_q - (1.0 - SMOOTH) * (a[2:3] + b[2:3]) - (SMOOTH / VALID_CLASSES) * (a[3:4] + b[3:4])
    small_ref[2:3, :] = jnp.broadcast_to(jnp.sum(loss, axis=1, keepdims=True) * (1.0 / rows_total), (1, width))
    small_ref[3:8, :] = jnp.zeros((5, width), jnp.float32)
    lse_own = spread_row(lse_of(d))
    dpool_ref[...] = jnp.zeros_like(dpool_ref)

    def dpool_step(k, carry):
        cols = col_ids(k)
        smooth = jnp.where(cols < VALID_CLASSES, SMOOTH / VALID_CLASSES, 0.0)
        soft = jnp.exp(logits[k] - repeat_lanes(lse_own, WCOLS))
        dl = (soft - jnp.where(repeat_lanes(labels, WCOLS) == cols, smooth + (1.0 - SMOOTH), smooth)) * (1.0 / rows_total)
        dpool_ref[...] += lax.dot_general(dl.astype(jnp.bfloat16), w_buf[k], (((1,), (1,)), ((), ())), preferred_element_type=jnp.float32)
        return carry

    lax.fori_loop(0, n_w, dpool_step, 0)
    for j in range(PIECES):
        third[j][0].wait_recv()
        third[j][1].wait_recv()
    fourth[3].start()
    for c in fourth[:3]:
        c.wait_recv()
    for c in flushes[3:7]:
        c.start()
    dpool = dpool_ref[...]
    part[0:1, :] = jnp.sum(dpool * pool[pl.ds(d * rows, rows), :], axis=0, keepdims=True)
    part[1:2, :] = jnp.sum(dpool, axis=0, keepdims=True)
    part_all[me] = part[...]

    def part_copy(k):
        return pltpu.make_async_remote_copy(src_ref=part, dst_ref=part_all.at[me], send_sem=dg_send_sem.at[k - 1], recv_sem=dg_recv_sem.at[k - 1], device_id=peer(k), device_id_type=pl.DeviceIdType.MESH)

    part_copies = [part_copy(k) for k in range(1, 16)]
    for c in part_copies:
        c.start()
    mi_copy.wait()
    lane_t = lax.broadcasted_iota(jnp.int32, (tokens, LANES), 1)
    mine = lane_t // half == t
    mean_ref[...] = jnp.where(mine, mean_ref[...], mi_recv[0])
    inv_ref[...] = jnp.where(mine, inv_ref[...], mi_recv[1])
    fourth[3].wait_recv()
    flushes[7].start()
    for c in part_copies:
        c.wait()
    small_ref[0:2, :] = jnp.sum(part_all[...], axis=0)
    for c in sum(first + second + third, []) + fourth:
        c.wait_send()
    for c in flushes:
        c.wait()


def front_call(feats, w_head, b_head, ln_gamma, ln_beta, labels, n_data):
    rows, tokens, width = feats.shape
    shard_cols = w_head.shape[1]
    n_w = shard_cols // WCOLS
    f32 = jnp.float32
    vmem = pl.BlockSpec(memory_space=pltpu.VMEM)
    anym = pl.BlockSpec(memory_space=pl.ANY)
    stat = jax.ShapeDtypeStruct((tokens, LANES), f32)
    return pl.pallas_call(
        front_kernel,
        name="front",
        in_specs=[anym, anym, vmem, vmem, vmem, vmem],
        out_specs=[anym] + [vmem] * 6,
        out_shape=[
            jax.ShapeDtypeStruct((rows * n_data, width), f32),
            stat,
            stat,
            jax.ShapeDtypeStruct((rows, width), f32),
            jax.ShapeDtypeStruct((8, LANES), f32),
            jax.ShapeDtypeStruct((8, LANES), f32),
            jax.ShapeDtypeStruct((8, width), f32),
        ],
        scratch_shapes=[
            pltpu.VMEM((SLOTS, GROUP, tokens, width), jnp.bfloat16),
            pltpu.VMEM((n_w, width, WCOLS), jnp.bfloat16),
            pltpu.VMEM((rows * n_data, width), f32),
            pltpu.VMEM((n_w, rows, WCOLS), f32),
            pltpu.VMEM((rows, width), jnp.bfloat16),
            pltpu.VMEM((8, LANES), f32),
            pltpu.VMEM((16, 8, LANES), f32),
            pltpu.VMEM((2, width), f32),
            pltpu.VMEM((16, 2, width), f32),
            pltpu.VMEM((2, tokens, LANES), f32),
            pltpu.VMEM((2, tokens, LANES), f32),
            pltpu.SemaphoreType.DMA((SLOTS,)),
            pltpu.SemaphoreType.DMA((n_w,)),
            pltpu.SemaphoreType.DMA((33,)),
            pltpu.SemaphoreType.DMA((33,)),
            pltpu.SemaphoreType.DMA((15,)),
            pltpu.SemaphoreType.DMA((15,)),
            pltpu.SemaphoreType.DMA((15,)),
            pltpu.SemaphoreType.DMA((15,)),
            pltpu.SemaphoreType.DMA((8,)),
        ],
        compiler_params=pltpu.CompilerParams(collective_id=0, has_side_effects=True, vmem_limit_bytes=63 * 2**20),
    )(feats, w_head, b_head.reshape(n_w, 1, WCOLS), ln_gamma, ln_beta, labels[None, :])


def fill_rows(pool_ref, gamma_ref, beta_ref, lse_ref, y_ref, p_ref, pt_ref, lse_b, y_b):
    rows, width = p_ref.shape

    @pl.when(pl.program_id(0) == 0)
    def _():
        def fill(r, carry):
            sl = pl.ds(r * LANES, LANES)
            p = pool_ref[sl, :] * gamma_ref[...].reshape(1, width) + beta_ref[...].reshape(1, width)
            p_ref[sl, :] = p.astype(jnp.bfloat16)
            lse_b[sl, :] = spread_row(lse_ref[pl.ds(r, 1), :] + math.log(rows))
            y_b[sl, :] = spread_row(y_ref[pl.ds(r, 1), :]).astype(jnp.int32)
            return carry

        lax.fori_loop(0, rows // LANES, fill, 0)
        for r in range(rows // LANES):
            pt_ref[:, r * LANES:(r + 1) * LANES] = p_ref[r * LANES:(r + 1) * LANES, :].T


def soft_piece(base, s, part, logits, rows_total, lse_b, y_b, b_ref, db_ref, dl_ref, fresh):
    sub = pl.ds(s * SUB, SUB)
    col = base + s * SUB + lax.broadcasted_iota(jnp.int32, (1, SUB), 1)
    valid = col < VALID_CLASSES
    smooth = jnp.where(valid, SMOOTH / VALID_CLASSES / rows_total, 0.0)
    target = smooth + (1.0 - SMOOTH) / rows_total
    bias = jnp.where(valid, b_ref[:, sub], -jnp.inf)
    soft = jnp.exp((logits + bias) - repeat_lanes(lse_b[part, :], SUB))
    dlogit = soft - jnp.where(repeat_lanes(y_b[part, :], SUB) == col, target, smooth)
    db = jnp.sum(dlogit, axis=0, keepdims=True)
    db_ref[:, sub] = db if fresh else db_ref[:, sub] + db
    dl_ref[s, part, :] = dlogit.astype(jnp.bfloat16)


def head_kernel(shard_cols, pool_ref, gamma_ref, beta_ref, lse_ref, y_ref, w_ref, b_ref, dw_ref, db_ref, p_ref, pt_ref, lse_b, y_b, dl_ref):
    fill_rows(pool_ref, gamma_ref, beta_ref, lse_ref, y_ref, p_ref, pt_ref, lse_b, y_b)
    rows = p_ref.shape[0]
    cols = w_ref.shape[1]
    base = lax.axis_index("tp") * shard_cols + pl.program_id(0) * cols
    every = pl.ds(0, rows)

    def first_half(s):
        logits = jnp.dot(p_ref[...], w_ref[:, pl.ds(s * SUB, SUB)], preferred_element_type=jnp.float32)
        soft_piece(base, s, every, logits, rows, lse_b, y_b, b_ref, db_ref, dl_ref, True)

    def second_half(s):
        dw_ref[:, pl.ds(s * SUB, SUB)] = jnp.dot(pt_ref[...], dl_ref[s], preferred_element_type=jnp.float32)

    first_half(0)
    for s in range(1, cols // SUB):
        first_half(s)
        second_half(s - 1)
    second_half(cols // SUB - 1)


def feat_image(i, x_ref, mean_t, inv_t, u_ref, df_ref):
    imgs, tokens, width = x_ref.shape
    u = u_ref[pl.ds(i, 1), :]
    um = jnp.broadcast_to(jnp.sum(u, axis=1, keepdims=True) * (1.0 / width), (ROW_TILE, LANES))
    for c in range(tokens // ROW_TILE):
        rows = pl.ds(c * ROW_TILE, ROW_TILE)
        mean = jnp.broadcast_to(mean_t[rows, i:i + 1], (ROW_TILE, LANES))
        inv = jnp.broadcast_to(inv_t[rows, i:i + 1], (ROW_TILE, LANES))
        x = x_ref[i, rows, :].astype(jnp.float32)

        dots = jnp.broadcast_to(jnp.sum(x * u, axis=1, keepdims=True), (ROW_TILE, LANES))
        slope = -(inv * inv * inv) * (dots * (1.0 / width) - mean * um)
        offset = -(inv * um) - slope * mean
        x = x_ref[i, rows, :].astype(jnp.float32)
        df_ref[i, rows, :] = (x * repeat_lanes(slope, width) + (u * repeat_lanes(inv, width) + repeat_lanes(offset, width))).astype(jnp.bfloat16)


def head_feat_kernel(shard_cols, skip_cols, pool_ref, gamma_ref, beta_ref, lse_ref, y_ref, w_ref, b_ref, x_ref, mean_ref, inv_ref, own_ref, other_ref, small_ref, dw_in, db_in,
                     dw_ref, db_ref, df_ref, dgamma_ref, dbeta_ref, loss_ref, p_ref, pt_ref, lse_b, y_b, dl_ref, mean_t, inv_t, u_ref):
    imgs, tokens, width = x_ref.shape
    rows = p_ref.shape[0]
    cols = w_ref.shape[1]
    step = pl.program_id(0)
    fill_rows(pool_ref, gamma_ref, beta_ref, lse_ref, y_ref, p_ref, pt_ref, lse_b, y_b)

    @pl.when(step == 0)
    def _():
        dgamma_ref[...] = small_ref[0:1, :].reshape(width)
        dbeta_ref[...] = small_ref[1:2, :].reshape(width)
        loss_ref[...] = small_ref[2:3, 0:1]

    turn = (LANES - step * imgs) % LANES
    mean_t[...] = pltpu.roll(mean_ref[...], turn, axis=1)
    inv_t[...] = pltpu.roll(inv_ref[...], turn, axis=1)
    u_ref[...] = (own_ref[...] + other_ref[...]) * gamma_ref[...].reshape(1, width) * (1.0 / tokens)
    base = lax.axis_index("tp") * shard_cols + skip_cols + step * cols
    def first_half(s, m):
        part = pl.ds(m * (rows // PARTS), rows // PARTS)
        logits = jnp.dot(p_ref[part, :], w_ref[:, pl.ds(s * SUB, SUB)], preferred_element_type=jnp.float32)
        soft_piece(base, s, part, logits, rows, lse_b, y_b, b_ref, db_ref, dl_ref, m == 0)

    def second_half(s, m):
        part = pl.ds(m * (width // PARTS), width // PARTS)
        dw_ref[part, pl.ds(s * SUB, SUB)] = jnp.dot(pt_ref[part, :], dl_ref[s], preferred_element_type=jnp.float32)

    order = [(first_half, 0, m) for m in range(PARTS)]
    for s in range(1, cols // SUB):
        order += [(first_half, s, m) for m in range(PARTS)]
        order += [(second_half, s - 1, m) for m in range(PARTS)]
    order += [(second_half, cols // SUB - 1, m) for m in range(PARTS)]
    for n, (run, s, m) in enumerate(order):
        run(s, m)
        for i in range(n * imgs // len(order), (n + 1) * imgs // len(order)):
            feat_image(i, x_ref, mean_t, inv_t, u_ref, df_ref)


def resident(shape):
    return pl.BlockSpec(shape, lambda g: (0,) * len(shape), pipeline_mode=pl.Buffered(1))


def head_calls(pool, ln_gamma, ln_beta, lse_all, y_all, w_head, b_head, feats, mean, inv, own, other, small):
    rows, width = pool.shape
    shard_cols = w_head.shape[1]
    imgs_all, tokens, _ = feats.shape
    feat_steps = imgs_all // IMGS
    skip_cols = shard_cols - feat_steps * COLS
    f32 = jnp.float32
    args = (pool, ln_gamma, ln_beta, lse_all, y_all, w_head, b_head[None, :])
    dw_shape = jax.ShapeDtypeStruct((width, shard_cols), f32)
    db_shape = jax.ShapeDtypeStruct((1, shard_cols), f32)

    def scratch(cols):
        return [
            pltpu.VMEM((rows, width), jnp.bfloat16),
            pltpu.VMEM((width, rows), jnp.bfloat16),
            pltpu.VMEM((rows, LANES), f32),
            pltpu.VMEM((rows, LANES), jnp.int32),
            pltpu.VMEM((cols // SUB, rows, SUB), jnp.bfloat16),
        ]

    def outs(cols, skip):
        return [pl.BlockSpec((width, cols), lambda g: (0, g + skip // cols)), pl.BlockSpec((1, cols), lambda g: (0, g + skip // cols))]

    def specs(cols, skip):
        return [
            resident((rows, width)),
            resident((width,)),
            resident((width,)),
            resident((8, LANES)),
            resident((8, LANES)),
            pl.BlockSpec((width, cols), lambda g: (0, g + skip // cols)),
            pl.BlockSpec((1, cols), lambda g: (0, g + skip // cols)),
        ]

    def cost(cols):
        return pl.CostEstimate(flops=4 * rows * width * cols, bytes_accessed=6 * width * cols, transcendentals=rows * cols)

    params = pltpu.CompilerParams(vmem_limit_bytes=56 * 2**20)
    dw, db = pl.pallas_call(
        functools.partial(head_kernel, shard_cols),
        name="head",
        grid=(skip_cols // LEAD_COLS,),
        in_specs=specs(LEAD_COLS, 0),
        out_specs=outs(LEAD_COLS, 0),
        out_shape=[dw_shape, db_shape],
        scratch_shapes=scratch(LEAD_COLS),
        compiler_params=params,
        cost_estimate=cost(skip_cols),
    )(*args)
    img = lambda shape: pl.BlockSpec(shape, lambda g: (g,) + (0,) * (len(shape) - 1))
    n_in = 13
    dw, db, df, dgamma, dbeta, loss = pl.pallas_call(
        functools.partial(head_feat_kernel, shard_cols, skip_cols),
        name="head_feat",
        grid=(feat_steps,),
        in_specs=specs(COLS, skip_cols)
        + [img((IMGS, tokens, width)), resident((tokens, LANES)), resident((tokens, LANES)), img((IMGS, width)), img((IMGS, width)), resident(small.shape)]
        + [pl.BlockSpec(memory_space=pl.ANY)] * 2,
        out_specs=outs(COLS, skip_cols)
        + [img((IMGS, tokens, width)), pl.BlockSpec((width,), lambda g: (0,)), pl.BlockSpec((width,), lambda g: (0,)), pl.BlockSpec((1, 1), lambda g: (0, 0))],
        out_shape=[
            dw_shape,
            db_shape,
            jax.ShapeDtypeStruct(feats.shape, jnp.bfloat16),
            jax.ShapeDtypeStruct((width,), f32),
            jax.ShapeDtypeStruct((width,), f32),
            jax.ShapeDtypeStruct((1, 1), f32),
        ],
        scratch_shapes=scratch(COLS)
        + [pltpu.VMEM((tokens, LANES), f32)] * 2
        + [pltpu.VMEM((IMGS, width), f32)],
        input_output_aliases={n_in: 0, n_in + 1: 1},
        compiler_params=pltpu.CompilerParams(vmem_limit_bytes=56 * 2**20),
        cost_estimate=cost(shard_cols - skip_cols),
    )(*args, feats, mean, inv, own, other, small, dw, db)
    return dw, db[0], df, dgamma, dbeta, loss[0, 0]


def solution(mesh):
    n_data = mesh.shape["dp"]

    def local_head(feats, ln_gamma, ln_beta, w_head, b_head, labels):
        pool, mean, inv, dpool, lse_all, y_all, small = front_call(feats, w_head, b_head, ln_gamma, ln_beta, labels, n_data)
        dpool_other = lax.ppermute(dpool, "tp", [(0, 1), (1, 0)])
        dw, db, df, dgamma, dbeta, loss = head_calls(pool, ln_gamma, ln_beta, lse_all, y_all, w_head, b_head, feats, mean, inv, dpool, dpool_other, small)
        return loss, df, dw, db, dgamma, dbeta

    return jax.shard_map(local_head, mesh=mesh, in_specs=(P("dp", None, None), P(), P(), P(None, "tp"), P("tp"), P("dp")), out_specs=(P(), P("dp", None, None), P(None, "tp"), P("tp"), P(), P()), check_vma=False)
```

```python
import functools
import math

import jax
import jax.numpy as jnp
from jax import lax
from jax.experimental import pallas as pl
from jax.experimental.pallas import tpu as pltpu
from jax.sharding import PartitionSpec as P

VALID_CLASSES = 21841
LN_EPS = 1e-5
SMOOTH = 0.1
LANES = 128
COLS = 512
LEAD_COLS = 1024
SUB = 256
IMGS = 8
ROW_TILE = 16
GROUP = 4
WCOLS = 1024
SLOTS = 3
PIECES = 4
PARTS = 2


def repeat_lanes(tile, width):
    return jnp.concatenate([tile] * (width // LANES), axis=1)


def fold_lanes(x, op):
    tiles = [x[:, j * LANES:(j + 1) * LANES] for j in range(x.shape[1] // LANES)]
    return functools.reduce(op, tiles)


def spread_row(row):
    return jnp.broadcast_to(row, (LANES, LANES)).T


def norm_image(x_ref, slot, i, lane_id, pool_row, pool_ref, mean_ref, inv_ref):
    _, _, tokens, width = x_ref.shape
    chunks = tokens // ROW_TILE
    lane = lax.broadcasted_iota(jnp.int32, (ROW_TILE, LANES), 1)
    means, invs = [], []
    for c in range(chunks):
        x = x_ref[slot, i, pl.ds(c * ROW_TILE, ROW_TILE), :].astype(jnp.float32)
        means.append(jnp.sum(x, axis=1, keepdims=True) * (1.0 / width))
    for c in range(chunks):
        x = x_ref[slot, i, pl.ds(c * ROW_TILE, ROW_TILE), :].astype(jnp.float32) - means[c]
        var = jnp.sum(x * x, axis=1, keepdims=True) * (1.0 / width)
        invs.append(lax.rsqrt(var + LN_EPS))
    total = jnp.zeros((ROW_TILE, width), jnp.float32)
    shift = jnp.zeros((ROW_TILE, 1), jnp.float32)
    for c in range(chunks):
        x = x_ref[slot, i, pl.ds(c * ROW_TILE, ROW_TILE), :].astype(jnp.float32)
        total = total + x * invs[c]
        shift = shift + means[c] * invs[c]
        rows = pl.ds(c * ROW_TILE, ROW_TILE)
        mean_ref[rows, :] = jnp.where(lane == lane_id, means[c], mean_ref[rows, :])
        inv_ref[rows, :] = jnp.where(lane == lane_id, invs[c], inv_ref[rows, :])
    pool_ref[pl.ds(pool_row, 1), :] = jnp.sum(total - shift, axis=0, keepdims=True) * (1.0 / tokens)


def front_kernel(x_hbm, w_hbm, b_ref, gamma_ref, beta_ref, y_ref,
                 pool_out, mean_ref, inv_ref, dpool_ref, lse_ref, yf_ref, small_ref,
                 x_buf, w_buf, pool, logits, p16, stat_send, stat_recv, part, part_all, mi_send, mi_recv,
                 x_sem, w_sem, send_sem, recv_sem, st_send_sem, st_recv_sem, dg_send_sem, dg_recv_sem, out_sem):
    rows, tokens, width = x_hbm.shape
    half = rows // 2
    quarter = half // PIECES
    shard_cols = w_hbm.shape[1]
    n_w = shard_cols // WCOLS
    groups = half // GROUP
    rows_total = pool.shape[0]
    t = lax.axis_index("tp")
    d = lax.axis_index("dp")
    me = t * 8 + d
    dx = d + 2 - 4 * ((d // 2) % 2)
    dy = d + 4 - 8 * (d // 4)
    dxy = dx + 4 - 8 * (d // 4)

    def sibling(q):
        return q + 1 - 2 * (q % 2)

    def peer(k):
        q = (me + k) % 16
        return {"tp": q // 8, "dp": q % 8}

    barrier = pltpu.get_barrier_semaphore()
    for k in range(1, 16):
        pl.semaphore_signal(barrier, inc=1, device_id=peer(k), device_id_type=pl.DeviceIdType.MESH)

    def x_copy(g, slot):
        return pltpu.make_async_copy(x_hbm.at[pl.ds(t * half + g * GROUP, GROUP)], x_buf.at[slot], x_sem.at[slot])

    def w_copy(k):
        return pltpu.make_async_copy(w_hbm.at[:, pl.ds(k * WCOLS, WCOLS)], w_buf.at[k], w_sem.at[k])

    def chunk(q, tt, h):
        return pool.at[pl.ds(q * rows + tt * half + h * quarter, quarter)]

    def remote(ref, sem, target):
        return pltpu.make_async_remote_copy(src_ref=ref, dst_ref=ref, send_sem=send_sem.at[sem], recv_sem=recv_sem.at[sem], device_id=target, device_id_type=pl.DeviceIdType.MESH)

    to_z = {"tp": 1 - t, "dp": d}
    to_x = {"tp": t, "dp": dx}
    to_y = {"tp": t, "dp": dy}
    to_c = {"tp": t, "dp": sibling(d)}

    x_copy(0, 0).start()
    x_copy(1, 1).start()
    mean_ref[...] = jnp.zeros_like(mean_ref)
    inv_ref[...] = jnp.zeros_like(inv_ref)

    def do_group(g, carry):
        slot = g % SLOTS
        x_copy(g, slot).wait()

        @pl.when(g + 2 < groups)
        def _():
            x_copy(g + 2, (g + 2) % SLOTS).start()

        @pl.when(g % 3 != 2)
        def _():
            w_copy(g - g // 3).start()

        def image(i, c):
            local = t * half + g * GROUP + i
            norm_image(x_buf, slot, i, local, d * rows + local, pool, mean_ref, inv_ref)
            return c

        lax.fori_loop(0, GROUP, image, 0)
        return carry

    first = [[remote(chunk(d, t, j), 3 * j + a, to) for a, to in enumerate((to_z, to_x, to_y))] for j in range(PIECES)]
    second = [[remote(chunk(d, 1 - t, j), 12 + 2 * j + a, to) for a, to in enumerate((to_x, to_y))] for j in range(PIECES)]
    third = [remote(chunk(dx, t, j), 20 + j, to_y) if j % 2 == 0 else remote(chunk(dy, t, j), 20 + j, to_x) for j in range(PIECES)]
    fifth = [remote(chunk(dxy, t, j), 24 + j, to_z) for j in range(PIECES)]

    def block(q):
        return pool.at[pl.ds(q * rows, rows)]

    fourth = [remote(block(q), 28 + j, to_c) for j, q in enumerate((d, dx, dy, dxy))]
    mi_copy = pltpu.make_async_remote_copy(src_ref=mi_send, dst_ref=mi_recv, send_sem=send_sem.at[32], recv_sem=recv_sem.at[32], device_id=to_z, device_id_type=pl.DeviceIdType.MESH)

    def flush(j, q):
        return pltpu.make_async_copy(block(q), pool_out.at[pl.ds(q * rows, rows)], out_sem.at[j])

    flushes = [flush(j, q) for j, q in enumerate((d, dx, dy, dxy, sibling(d), sibling(dx), sibling(dy), sibling(dxy)))]

    def pass_z(j):
        first[j][0].wait_recv()
        for c in second[j]:
            c.start()

    def pass_side(j):
        first[j][1 + j % 2].wait_recv()
        third[j].start()

    def pass_diagonal(j):
        third[j].wait_recv()
        fifth[j].start()

    for j in range(PIECES):
        lax.fori_loop(j * groups // PIECES, (j + 1) * groups // PIECES, do_group, 0)
        if j == 0:
            pl.semaphore_wait(barrier, 15)
        if j == PIECES - 1:
            mi_send[0] = mean_ref[...]
            mi_send[1] = inv_ref[...]
        for c in first[j]:
            c.start()
        if j >= 1:
            pass_z(j - 1)
            pass_side(j - 1)
        if j >= 2:
            pass_diagonal(j - 2)
    pass_z(PIECES - 1)
    fourth[0].start()
    gamma = gamma_ref[...].reshape(1, width)
    beta = beta_ref[...].reshape(1, width)
    p16[...] = (pool[pl.ds(d * rows, rows), :] * gamma + beta).astype(jnp.bfloat16)

    def col_ids(k):
        return t * shard_cols + k * WCOLS + lax.broadcasted_iota(jnp.int32, (1, WCOLS), 1)

    def logits_step(k, top):
        w_copy(k).wait()
        cols = col_ids(k)
        bias = jnp.where(cols < VALID_CLASSES, b_ref[k], -jnp.inf)
        out = jnp.dot(p16[...], w_buf[k], preferred_element_type=jnp.float32) + bias
        logits[k] = out
        return jnp.maximum(top, fold_lanes(out, jnp.maximum))

    top = lax.fori_loop(0, n_w // 2, logits_step, jnp.full((rows, LANES), -jnp.inf, jnp.float32))
    mi_copy.start()
    pass_side(PIECES - 1)
    pass_diagonal(PIECES - 2)
    top = lax.fori_loop(n_w // 2, n_w, logits_step, top)
    pass_diagonal(PIECES - 1)
    for j in range(PIECES):
        first[j][2 - j % 2].wait_recv()
        second[j][0].wait_recv()
        second[j][1].wait_recv()
    fourth[1].start()
    fourth[2].start()
    row_top = jnp.broadcast_to(jnp.max(top, axis=1, keepdims=True), (rows, LANES))
    labels_f = spread_row(y_ref[...].astype(jnp.float32))
    labels = labels_f.astype(jnp.int32)
    zero = jnp.zeros((rows, LANES), jnp.float32)

    def stat_step(k, carry):
        total, target, valid_sum = carry
        cols = col_ids(k)
        out = logits[k]
        e = jnp.exp(out - repeat_lanes(row_top, WCOLS))
        hit = jnp.where(repeat_lanes(labels, WCOLS) == cols, out, 0.0)
        ok = jnp.where(cols < VALID_CLASSES, out, 0.0)
        return total + fold_lanes(e, jnp.add), target + fold_lanes(hit, jnp.add), valid_sum + fold_lanes(ok, jnp.add)

    total, target, valid_sum = lax.fori_loop(0, n_w, stat_step, (zero, zero, zero))
    lane = lax.broadcasted_iota(jnp.int32, (rows, LANES), 1)
    packed = jnp.where(lane == 0, row_top, jnp.where(lane == 1, jnp.sum(total, axis=1, keepdims=True), jnp.where(lane == 2, jnp.sum(target, axis=1, keepdims=True), jnp.where(lane == 3, jnp.sum(valid_sum, axis=1, keepdims=True), labels_f))))
    stat_send[...] = packed.T[:8]
    stat_recv[me] = stat_send[...]

    def stat_copy(k):
        return pltpu.make_async_remote_copy(src_ref=stat_send, dst_ref=stat_recv.at[me], send_sem=st_send_sem.at[k - 1], recv_sem=st_recv_sem.at[k - 1], device_id=peer(k), device_id_type=pl.DeviceIdType.MESH)

    stat_copies = [stat_copy(k) for k in range(1, 16)]
    for c in stat_copies:
        c.start()
    for c in flushes[:3]:
        c.start()
    for c in stat_copies:
        c.wait()

    def lse_of(q):
        a, b = stat_recv[q], stat_recv[8 + q]
        hi = jnp.maximum(a[0:1], b[0:1])
        return hi + jnp.log(a[1:2] * jnp.exp(a[0:1] - hi) + b[1:2] * jnp.exp(b[0:1] - hi))

    loss = jnp.zeros((1, LANES), jnp.float32)
    for q in range(8):
        lse_q = lse_of(q)
        lse_ref[q:q + 1, :] = lse_q
        a, b = stat_recv[q], stat_recv[8 + q]
        yf_ref[q:q + 1, :] = a[4:5]
        loss = loss + lse_q - (1.0 - SMOOTH) * (a[2:3] + b[2:3]) - (SMOOTH / VALID_CLASSES) * (a[3:4] + b[3:4])
    small_ref[2:3, :] = jnp.broadcast_to(jnp.sum(loss, axis=1, keepdims=True) * (1.0 / rows_total), (1, width))
    small_ref[3:8, :] = jnp.zeros((5, width), jnp.float32)
    lse_own = spread_row(lse_of(d))
    dpool_ref[...] = jnp.zeros_like(dpool_ref)

    def dpool_step(k, carry):
        cols = col_ids(k)
        smooth = jnp.where(cols < VALID_CLASSES, SMOOTH / VALID_CLASSES, 0.0)
        soft = jnp.exp(logits[k] - repeat_lanes(lse_own, WCOLS))
        dl = (soft - jnp.where(repeat_lanes(labels, WCOLS) == cols, smooth + (1.0 - SMOOTH), smooth)) * (1.0 / rows_total)
        dpool_ref[...] += lax.dot_general(dl.astype(jnp.bfloat16), w_buf[k], (((1,), (1,)), ((), ())), preferred_element_type=jnp.float32)
        return carry

    lax.fori_loop(0, n_w, dpool_step, 0)
    for j in range(PIECES):
        fifth[j].wait_recv()
    fourth[3].start()
    for c in fourth[:3]:
        c.wait_recv()
    for c in flushes[3:7]:
        c.start()
    dpool = dpool_ref[...]
    part[0:1, :] = jnp.sum(dpool * pool[pl.ds(d * rows, rows), :], axis=0, keepdims=True)
    part[1:2, :] = jnp.sum(dpool, axis=0, keepdims=True)
    part_all[me] = part[...]

    def part_copy(k):
        return pltpu.make_async_remote_copy(src_ref=part, dst_ref=part_all.at[me], send_sem=dg_send_sem.at[k - 1], recv_sem=dg_recv_sem.at[k - 1], device_id=peer(k), device_id_type=pl.DeviceIdType.MESH)

    part_copies = [part_copy(k) for k in range(1, 16)]
    for c in part_copies:
        c.start()
    mi_copy.wait()
    lane_t = lax.broadcasted_iota(jnp.int32, (tokens, LANES), 1)
    mine = lane_t // half == t
    mean_ref[...] = jnp.where(mine, mean_ref[...], mi_recv[0])
    inv_ref[...] = jnp.where(mine, inv_ref[...], mi_recv[1])
    fourth[3].wait_recv()
    flushes[7].start()
    for c in part_copies:
        c.wait()
    small_ref[0:2, :] = jnp.sum(part_all[...], axis=0)
    for c in sum(first + second, []) + third + fourth + fifth:
        c.wait_send()
    for c in flushes:
        c.wait()


def front_call(feats, w_head, b_head, ln_gamma, ln_beta, labels, n_data):
    rows, tokens, width = feats.shape
    shard_cols = w_head.shape[1]
    n_w = shard_cols // WCOLS
    f32 = jnp.float32
    vmem = pl.BlockSpec(memory_space=pltpu.VMEM)
    anym = pl.BlockSpec(memory_space=pl.ANY)
    stat = jax.ShapeDtypeStruct((tokens, LANES), f32)
    return pl.pallas_call(
        front_kernel,
        name="front",
        in_specs=[anym, anym, vmem, vmem, vmem, vmem],
        out_specs=[anym] + [vmem] * 6,
        out_shape=[
            jax.ShapeDtypeStruct((rows * n_data, width), f32),
            stat,
            stat,
            jax.ShapeDtypeStruct((rows, width), f32),
            jax.ShapeDtypeStruct((8, LANES), f32),
            jax.ShapeDtypeStruct((8, LANES), f32),
            jax.ShapeDtypeStruct((8, width), f32),
        ],
        scratch_shapes=[
            pltpu.VMEM((SLOTS, GROUP, tokens, width), jnp.bfloat16),
            pltpu.VMEM((n_w, width, WCOLS), jnp.bfloat16),
            pltpu.VMEM((rows * n_data, width), f32),
            pltpu.VMEM((n_w, rows, WCOLS), f32),
            pltpu.VMEM((rows, width), jnp.bfloat16),
            pltpu.VMEM((8, LANES), f32),
            pltpu.VMEM((16, 8, LANES), f32),
            pltpu.VMEM((2, width), f32),
            pltpu.VMEM((16, 2, width), f32),
            pltpu.VMEM((2, tokens, LANES), f32),
            pltpu.VMEM((2, tokens, LANES), f32),
            pltpu.SemaphoreType.DMA((SLOTS,)),
            pltpu.SemaphoreType.DMA((n_w,)),
            pltpu.SemaphoreType.DMA((33,)),
            pltpu.SemaphoreType.DMA((33,)),
            pltpu.SemaphoreType.DMA((15,)),
            pltpu.SemaphoreType.DMA((15,)),
            pltpu.SemaphoreType.DMA((15,)),
            pltpu.SemaphoreType.DMA((15,)),
            pltpu.SemaphoreType.DMA((8,)),
        ],
        compiler_params=pltpu.CompilerParams(collective_id=0, has_side_effects=True, vmem_limit_bytes=63 * 2**20),
    )(feats, w_head, b_head.reshape(n_w, 1, WCOLS), ln_gamma, ln_beta, labels[None, :])


def fill_rows(pool_ref, gamma_ref, beta_ref, lse_ref, y_ref, p_ref, pt_ref, lse_b, y_b):
    rows, width = p_ref.shape

    @pl.when(pl.program_id(0) == 0)
    def _():
        def fill(r, carry):
            sl = pl.ds(r * LANES, LANES)
            p = pool_ref[sl, :] * gamma_ref[...].reshape(1, width) + beta_ref[...].reshape(1, width)
            p_ref[sl, :] = p.astype(jnp.bfloat16)
            lse_b[sl, :] = spread_row(lse_ref[pl.ds(r, 1), :] + math.log(rows))
            y_b[sl, :] = spread_row(y_ref[pl.ds(r, 1), :]).astype(jnp.int32)
            return carry

        lax.fori_loop(0, rows // LANES, fill, 0)
        for r in range(rows // LANES):
            pt_ref[:, r * LANES:(r + 1) * LANES] = p_ref[r * LANES:(r + 1) * LANES, :].T


def soft_piece(base, s, part, logits, rows_total, lse_b, y_b, b_ref, db_ref, dl_ref, fresh):
    sub = pl.ds(s * SUB, SUB)
    col = base + s * SUB + lax.broadcasted_iota(jnp.int32, (1, SUB), 1)
    valid = col < VALID_CLASSES
    smooth = jnp.where(valid, SMOOTH / VALID_CLASSES / rows_total, 0.0)
    target = smooth + (1.0 - SMOOTH) / rows_total
    bias = jnp.where(valid, b_ref[:, sub], -jnp.inf)
    soft = jnp.exp((logits + bias) - repeat_lanes(lse_b[part, :], SUB))
    dlogit = soft - jnp.where(repeat_lanes(y_b[part, :], SUB) == col, target, smooth)
    db = jnp.sum(dlogit, axis=0, keepdims=True)
    db_ref[:, sub] = db if fresh else db_ref[:, sub] + db
    dl_ref[s, part, :] = dlogit.astype(jnp.bfloat16)


def head_kernel(shard_cols, pool_ref, gamma_ref, beta_ref, lse_ref, y_ref, w_ref, b_ref, dw_ref, db_ref, p_ref, pt_ref, lse_b, y_b, dl_ref):
    fill_rows(pool_ref, gamma_ref, beta_ref, lse_ref, y_ref, p_ref, pt_ref, lse_b, y_b)
    rows = p_ref.shape[0]
    cols = w_ref.shape[1]
    base = lax.axis_index("tp") * shard_cols + pl.program_id(0) * cols
    every = pl.ds(0, rows)

    def first_half(s):
        logits = jnp.dot(p_ref[...], w_ref[:, pl.ds(s * SUB, SUB)], preferred_element_type=jnp.float32)
        soft_piece(base, s, every, logits, rows, lse_b, y_b, b_ref, db_ref, dl_ref, True)

    def second_half(s):
        dw_ref[:, pl.ds(s * SUB, SUB)] = jnp.dot(pt_ref[...], dl_ref[s], preferred_element_type=jnp.float32)

    first_half(0)
    for s in range(1, cols // SUB):
        first_half(s)
        second_half(s - 1)
    second_half(cols // SUB - 1)


def feat_image(i, x_ref, mean_t, inv_t, u_ref, df_ref):
    imgs, tokens, width = x_ref.shape
    u = u_ref[pl.ds(i, 1), :]
    um = jnp.broadcast_to(jnp.sum(u, axis=1, keepdims=True) * (1.0 / width), (ROW_TILE, LANES))
    for c in range(tokens // ROW_TILE):
        rows = pl.ds(c * ROW_TILE, ROW_TILE)
        mean = jnp.broadcast_to(mean_t[rows, i:i + 1], (ROW_TILE, LANES))
        inv = jnp.broadcast_to(inv_t[rows, i:i + 1], (ROW_TILE, LANES))
        x = x_ref[i, rows, :].astype(jnp.float32)

        dots = jnp.broadcast_to(jnp.sum(x * u, axis=1, keepdims=True), (ROW_TILE, LANES))
        slope = -(inv * inv * inv) * (dots * (1.0 / width) - mean * um)
        offset = -(inv * um) - slope * mean
        x = x_ref[i, rows, :].astype(jnp.float32)
        df_ref[i, rows, :] = (x * repeat_lanes(slope, width) + (u * repeat_lanes(inv, width) + repeat_lanes(offset, width))).astype(jnp.bfloat16)


def head_feat_kernel(shard_cols, skip_cols, pool_ref, gamma_ref, beta_ref, lse_ref, y_ref, w_ref, b_ref, x_ref, mean_ref, inv_ref, own_ref, other_ref, small_ref, dw_in, db_in,
                     dw_ref, db_ref, df_ref, dgamma_ref, dbeta_ref, loss_ref, p_ref, pt_ref, lse_b, y_b, dl_ref, mean_t, inv_t, u_ref):
    imgs, tokens, width = x_ref.shape
    rows = p_ref.shape[0]
    cols = w_ref.shape[1]
    step = pl.program_id(0)
    fill_rows(pool_ref, gamma_ref, beta_ref, lse_ref, y_ref, p_ref, pt_ref, lse_b, y_b)

    @pl.when(step == 0)
    def _():
        dgamma_ref[...] = small_ref[0:1, :].reshape(width)
        dbeta_ref[...] = small_ref[1:2, :].reshape(width)
        loss_ref[...] = small_ref[2:3, 0:1]

    turn = (LANES - step * imgs) % LANES
    mean_t[...] = pltpu.roll(mean_ref[...], turn, axis=1)
    inv_t[...] = pltpu.roll(inv_ref[...], turn, axis=1)
    u_ref[...] = (own_ref[...] + other_ref[...]) * gamma_ref[...].reshape(1, width) * (1.0 / tokens)
    base = lax.axis_index("tp") * shard_cols + skip_cols + step * cols
    def first_half(s, m):
        part = pl.ds(m * (rows // PARTS), rows // PARTS)
        logits = jnp.dot(p_ref[part, :], w_ref[:, pl.ds(s * SUB, SUB)], preferred_element_type=jnp.float32)
        soft_piece(base, s, part, logits, rows, lse_b, y_b, b_ref, db_ref, dl_ref, m == 0)

    def second_half(s, m):
        part = pl.ds(m * (width // PARTS), width // PARTS)
        dw_ref[part, pl.ds(s * SUB, SUB)] = jnp.dot(pt_ref[part, :], dl_ref[s], preferred_element_type=jnp.float32)

    order = [(first_half, 0, m) for m in range(PARTS)]
    for s in range(1, cols // SUB):
        order += [(first_half, s, m) for m in range(PARTS)]
        order += [(second_half, s - 1, m) for m in range(PARTS)]
    order += [(second_half, cols // SUB - 1, m) for m in range(PARTS)]
    for n, (run, s, m) in enumerate(order):
        run(s, m)
        for i in range(n * imgs // len(order), (n + 1) * imgs // len(order)):
            feat_image(i, x_ref, mean_t, inv_t, u_ref, df_ref)


def resident(shape):
    return pl.BlockSpec(shape, lambda g: (0,) * len(shape), pipeline_mode=pl.Buffered(1))


def head_calls(pool, ln_gamma, ln_beta, lse_all, y_all, w_head, b_head, feats, mean, inv, own, other, small):
    rows, width = pool.shape
    shard_cols = w_head.shape[1]
    imgs_all, tokens, _ = feats.shape
    feat_steps = imgs_all // IMGS
    skip_cols = shard_cols - feat_steps * COLS
    f32 = jnp.float32
    args = (pool, ln_gamma, ln_beta, lse_all, y_all, w_head, b_head[None, :])
    dw_shape = jax.ShapeDtypeStruct((width, shard_cols), f32)
    db_shape = jax.ShapeDtypeStruct((1, shard_cols), f32)

    def scratch(cols):
        return [
            pltpu.VMEM((rows, width), jnp.bfloat16),
            pltpu.VMEM((width, rows), jnp.bfloat16),
            pltpu.VMEM((rows, LANES), f32),
            pltpu.VMEM((rows, LANES), jnp.int32),
            pltpu.VMEM((cols // SUB, rows, SUB), jnp.bfloat16),
        ]

    def outs(cols, skip):
        return [pl.BlockSpec((width, cols), lambda g: (0, g + skip // cols)), pl.BlockSpec((1, cols), lambda g: (0, g + skip // cols))]

    def specs(cols, skip):
        return [
            resident((rows, width)),
            resident((width,)),
            resident((width,)),
            resident((8, LANES)),
            resident((8, LANES)),
            pl.BlockSpec((width, cols), lambda g: (0, g + skip // cols)),
            pl.BlockSpec((1, cols), lambda g: (0, g + skip // cols)),
        ]

    def cost(cols):
        return pl.CostEstimate(flops=4 * rows * width * cols, bytes_accessed=6 * width * cols, transcendentals=rows * cols)

    params = pltpu.CompilerParams(vmem_limit_bytes=56 * 2**20)
    dw, db = pl.pallas_call(
        functools.partial(head_kernel, shard_cols),
        name="head",
        grid=(skip_cols // LEAD_COLS,),
        in_specs=specs(LEAD_COLS, 0),
        out_specs=outs(LEAD_COLS, 0),
        out_shape=[dw_shape, db_shape],
        scratch_shapes=scratch(LEAD_COLS),
        compiler_params=pltpu.CompilerParams(vmem_limit_bytes=56 * 2**20),
        cost_estimate=cost(skip_cols),
    )(*args)
    img = lambda shape: pl.BlockSpec(shape, lambda g: (g,) + (0,) * (len(shape) - 1))
    n_in = 13
    dw, db, df, dgamma, dbeta, loss = pl.pallas_call(
        functools.partial(head_feat_kernel, shard_cols, skip_cols),
        name="head_feat",
        grid=(feat_steps,),
        in_specs=specs(COLS, skip_cols)
        + [img((IMGS, tokens, width)), resident((tokens, LANES)), resident((tokens, LANES)), img((IMGS, width)), img((IMGS, width)), resident(small.shape)]
        + [pl.BlockSpec(memory_space=pl.ANY)] * 2,
        out_specs=outs(COLS, skip_cols)
        + [img((IMGS, tokens, width)), pl.BlockSpec((width,), lambda g: (0,)), pl.BlockSpec((width,), lambda g: (0,)), pl.BlockSpec((1, 1), lambda g: (0, 0))],
        out_shape=[
            dw_shape,
            db_shape,
            jax.ShapeDtypeStruct(feats.shape, jnp.bfloat16),
            jax.ShapeDtypeStruct((width,), f32),
            jax.ShapeDtypeStruct((width,), f32),
            jax.ShapeDtypeStruct((1, 1), f32),
        ],
        scratch_shapes=scratch(COLS)
        + [pltpu.VMEM((tokens, LANES), f32)] * 2
        + [pltpu.VMEM((IMGS, width), f32)],
        input_output_aliases={n_in: 0, n_in + 1: 1},
        compiler_params=pltpu.CompilerParams(vmem_limit_bytes=56 * 2**20),
        cost_estimate=cost(shard_cols - skip_cols),
    )(*args, feats, mean, inv, own, other, small, dw, db)
    return dw, db[0], df, dgamma, dbeta, loss[0, 0]


def solution(mesh):
    n_data = mesh.shape["dp"]

    def local_head(feats, ln_gamma, ln_beta, w_head, b_head, labels):
        pool, mean, inv, dpool, lse_all, y_all, small = front_call(feats, w_head, b_head, ln_gamma, ln_beta, labels, n_data)
        dpool_other = lax.ppermute(dpool, "tp", [(0, 1), (1, 0)])
        dw, db, df, dgamma, dbeta, loss = head_calls(pool, ln_gamma, ln_beta, lse_all, y_all, w_head, b_head, feats, mean, inv, dpool, dpool_other, small)
        return loss, df, dw, db, dgamma, dbeta

    return jax.shard_map(local_head, mesh=mesh, in_specs=(P("dp", None, None), P(), P(), P(None, "tp"), P("tp"), P("dp")), out_specs=(P(), P("dp", None, None), P(None, "tp"), P("tp"), P(), P()), check_vma=False)
```
